256 devices in a mesh: gx: 64 (over x, z_hi, y), gy: 4 (over z_lo, core).
Axes of the slice: x: 4, y: 4, z: 8 (z_hi: 4, z_lo: 2; z = z_hi * 2 + z_lo), core: 2. Of those that a mesh axis runs over, the one named last changes fastest.
Arguments:
- displacement: float32 [3, 192, 32, 128], P(None, 'gx', 'gy'), may hold values from -0.1 to 0.1
- velocity: float32 [3, 192, 32, 128], P(None, 'gx', 'gy'), may hold values from -0.6 to 0.6
- bone: int32 [192, 32, 128], P('gx', 'gy'), may hold values 0 or 1
- broken: int32 [4, 192, 32, 128], P(None, 'gx', 'gy'), may hold values from 0 to 65535, as said below
Outputs:
- velocity_end: float32 [3, 192, 32, 128], P(None, 'gx', 'gy')
- damage: float32 [192, 32, 128], P('gx', 'gy')
The draws below stay inside these ranges and needn't reach their ends.
Inputs may be any that keep to these rules, and one draw needn't show every extreme that they name: 1 marks bone, 0 void. `broken`: only the bits that flag bonds are used: bits 0 to 15 of word 0 and bits 0 to 14 of words 1 to 3.
All inputs are finite; a program needn't handle non-finite values. No bound on the sum of `bone` on one device may be relied on, other than what follows from the above.
Results may differ from the reference program's by a relative error of at most 0.000069.
Values sent between devices are 32-bit elements; how exact they have to be, the bound alone decides.
No kernel may reach another device: no remote copies, remote signals or barrier semaphores. Data moves between devices by JAX's collectives and lax.ppermute only.
A program may use at most 128 MiB of HBM per device.

```python
import jax
import jax.numpy as jnp
from jax import lax

NZ = 128
STEPS = 2
NX = 192
NY = 32


def draw_broken(key, part):
    subkeys = jax.random.split(jax.random.fold_in(key, 17), 12)
    packed = []
    for position in range(4):
        ceiling = 65536 if position == 0 else 32768
        merged = jax.random.randint(subkeys[3 * position], (NX, NY, NZ), 0, ceiling, dtype=jnp.int32)
        for repeat in range(1, 3):
            another = jax.random.randint(subkeys[3 * position + repeat], (NX, NY, NZ), 0, ceiling, dtype=jnp.int32)
            merged = jnp.bitwise_and(merged, another)
        packed.append(merged)
    return jnp.stack(packed)


def plant(result, key, least, high):
    place = [jax.random.randint(jax.random.fold_in(key, axis), (), 0, length) for axis, length in enumerate(result.shape)]
    longest = result.shape.index(max(result.shape))
    next_to = place[:longest] + [(place[longest] + 1) % result.shape[longest]] + place[longest + 1:]
    return result.at[tuple(place)].set(least).at[tuple(next_to)].set(high)


def block_scale(rng, shape, cuts, low, high):
    def one(dim, shards_of):
        heights = jax.random.uniform(jax.random.fold_in(jax.random.fold_in(rng, 6), dim), (shards_of,), jnp.float32, low / len(cuts), high / len(cuts))
        return jnp.repeat(jnp.exp(heights), shape[dim] // shards_of).reshape((-1,) + (1,) * (len(shape) - dim - 1))

    loudness = one(*cuts[0])
    for cut in cuts[1:]:
        loudness = loudness * one(*cut)
    return loudness


def scatter_about(key, extent, scale, reach, shards=(), kind=jnp.bfloat16):
    values = scale * jax.random.normal(key, extent, jnp.float32)
    if shards:
        values = values * block_scale(key, extent, shards, -0.22, 0.18)
    return jnp.clip(values, -reach, reach).astype(kind)


def setup_inputs(seed: int = 0) -> dict:
    keys = jax.random.split(jax.random.key(seed), 5)
    displacement = scatter_about(keys[0], (3, NX, NY, NZ), 0.025, 0.1, ((1, 64), (2, 4)), jnp.float32)
    velocity = scatter_about(keys[1], (3, NX, NY, NZ), 0.2, 0.6, ((1, 64), (2, 4)), jnp.float32)
    bone = plant((jax.random.randint(keys[2], (NX, NY, NZ), 0, 8) < 7).astype(jnp.int32), jax.random.fold_in(keys[2], 1), 0, 1)
    broken = draw_broken(jax.random.fold_in(keys[4], 71), 0)
    return {"displacement": displacement, "velocity": velocity, "bone": bone, "broken": broken}


BULK_TERM = -50.0
SHEAR_TERM = 1500.0
TIME_STEP = 0.1
STRETCH_CRITICAL = 0.04
STRETCH_WIDTH = 0.01
DIRECTION_EPS = 1e-06

def half_bonds():
    listed = []
    for step_x in range(0, 4):
        for step_y in range(-3, 4):
            for step_z in range(-3, 4):
                forward_half = step_x > 0 or (step_x == 0 and (step_y > 0 or (step_y == 0 and step_z > 0)))
                if forward_half and step_x * step_x + step_y * step_y + step_z * step_z <= 9:
                    listed.append((step_x, step_y, step_z))
    return listed

def flag_place(number):
    if number < 16:
        return (0, number)
    return (1 + (number - 16) // 15, (number - 16) % 15)

def reference(displacement, velocity, bone, broken):
    forward_bonds = half_bonds()
    table_rows = []
    for number, (step_x, step_y, step_z) in enumerate(forward_bonds):
        word_index, bit_index = flag_place(number)
        table_rows.append([step_x, step_y, step_z, word_index, bit_index])
    bond_table = jnp.array(table_rows, dtype=jnp.int32)
    size_x, size_y, size_z = bone.shape
    bone_field = bone.astype(jnp.float32)
    bone_padded = jnp.pad(bone_field, 3)[None]
    pad_three = ((0, 0), (3, 3), (3, 3), (3, 3))

    def corner(entry):
        return (jnp.int32(0), entry[0] + 3, entry[1] + 3, entry[2] + 3)

    def neighbour(padded, entry):
        return lax.dynamic_slice(padded, corner(entry), (padded.shape[0], size_x, size_y, size_z))

    def add_remote(remote_part, contrib, entry):
        window = lax.dynamic_slice(remote_part, corner(entry), contrib.shape)
        return lax.dynamic_update_slice(remote_part, window + contrib, corner(entry))

    def geometry(moved_padded, moved_field, entry):
        nearby = neighbour(moved_padded, entry)
        offset = entry[:3].astype(jnp.float32)
        rel_x = nearby[0] - moved_field[0] + offset[0]
        rel_y = nearby[1] - moved_field[1] + offset[1]
        rel_z = nearby[2] - moved_field[2] + offset[2]
        squared = rel_x * rel_x + rel_y * rel_y + rel_z * rel_z
        length = jnp.sqrt(squared)
        natural = jnp.sqrt(offset[0] * offset[0] + offset[1] * offset[1] + offset[2] * offset[2])
        extension = length - natural
        stretch = extension / natural
        flagged = jnp.bitwise_and(jnp.right_shift(broken[entry[3]], entry[4]), 1).astype(jnp.float32)
        intact = bone_field * neighbour(bone_padded, entry)[0] * (1.0 - flagged)
        weight = intact * jax.nn.sigmoid((STRETCH_CRITICAL - stretch) / STRETCH_WIDTH)
        spread = jnp.sqrt(squared + DIRECTION_EPS)
        unit = jnp.stack([rel_x / spread, rel_y / spread, rel_z / spread])
        return (intact, weight, stretch, extension, natural, unit)

    def bond_sums(moved_field):
        moved_padded = jnp.pad(moved_field, pad_three)

        def visit_bond(running, entry):
            local_part, remote_part = running
            intact, weight, stretch, extension, natural, unit = geometry(moved_padded, moved_field, entry)
            contrib = jnp.stack([weight * extension, intact * natural, weight * natural])
            return ((local_part + contrib, add_remote(remote_part, contrib, entry)), None)
        initial = (jnp.zeros((3, size_x, size_y, size_z), jnp.float32), jnp.zeros((3, size_x + 6, size_y + 6, size_z + 6), jnp.float32))
        (local_part, remote_part), ignored = lax.scan(visit_bond, initial, bond_table)
        return local_part + remote_part[:, 3:-3, 3:-3, 3:-3]

    def bond_forces(moved_field, scaled, inverse):
        moved_padded = jnp.pad(moved_field, pad_three)
        ratio_padded = jnp.pad(jnp.stack([scaled, inverse]), pad_three)

        def visit_bond(running, entry):
            local_part, remote_part = running
            intact, weight, stretch, extension, natural, unit = geometry(moved_padded, moved_field, entry)
            nearby = neighbour(ratio_padded, entry)
            magnitude = weight * (BULK_TERM * (scaled + nearby[0]) + SHEAR_TERM * stretch * (inverse + nearby[1]))
            contrib = magnitude[None] * unit
            return ((local_part + contrib, add_remote(remote_part, -contrib, entry)), None)
        initial = (jnp.zeros((3, size_x, size_y, size_z), jnp.float32), jnp.zeros((3, size_x + 6, size_y + 6, size_z + 6), jnp.float32))
        (local_part, remote_part), ignored = lax.scan(visit_bond, initial, bond_table)
        return local_part + remote_part[:, 3:-3, 3:-3, 3:-3]
    current = displacement
    current_speed = velocity
    for step_index in range(STEPS):
        totals = bond_sums(current)
        if step_index == 0:
            volume = jnp.maximum(totals[1], 1.0)
            inverse = 1.0 / volume
        dilatation = 3.0 * totals[0] / volume
        scaled = dilatation * inverse
        force_field = bond_forces(current, scaled, inverse)
        current_speed = current_speed + TIME_STEP * force_field
        if step_index < STEPS - 1:
            current = current + TIME_STEP * current_speed
    damage = 1.0 - totals[2] / volume
    return (current_speed, damage)
```

```python
import math

import jax
import jax.numpy as jnp
from jax import lax
from jax.experimental import pallas as pl
from jax.experimental.pallas import tpu as pltpu
from jax.sharding import PartitionSpec as P

STEPS = 2

BULK_TERM = -50.0
SHEAR_TERM = 1500.0
TIME_STEP = 0.1
STRETCH_CRITICAL = 0.04
STRETCH_WIDTH = 0.01
DIRECTION_EPS = 1e-06

REACH = 3
HALF = 0.5 / STRETCH_WIDTH
PEN = 0.5 * STRETCH_CRITICAL / STRETCH_WIDTH
LOST = 1024.0
F32 = jnp.float32
VMEM_LIMIT = 20 * 1024 * 1024


def half_bonds():
    listed = []
    for step_x in range(0, 4):
        for step_y in range(-3, 4):
            for step_z in range(-3, 4):
                forward_half = step_x > 0 or (
                    step_x == 0 and (step_y > 0 or (step_y == 0 and step_z > 0))
                )
                if forward_half and step_x * step_x + step_y * step_y + step_z * step_z <= 9:
                    listed.append((step_x, step_y, step_z))
    return listed


def flag_place(number):
    if number < 16:
        return (0, number)
    return (1 + (number - 16) // 15, (number - 16) % 15)


def bond_classes():
    classes = {}
    for number, (a, b, c) in enumerate(half_bonds()):
        word, bit = flag_place(number)
        group = classes.setdefault(a * a + b * b + c * c, [])
        group.append((a, b, c, word, bit, False))
        group.append((-a, -b, -c, word, bit, True))
    place = 0
    for squared in sorted(classes):
        classes[squared] = [bond + (place + k,) for k, bond in enumerate(classes[squared])]
        place += len(classes[squared])
    return {squared: classes[squared] for squared in sorted(classes)}, place


CLASSES, BONDS = bond_classes()


def pairwise(values, axis, size, odd):
    pairs = []
    for i in range(1 if odd else 0, size - 1, 2):
        pairs += [(i, i + 1), (i + 1, i)]
    return lax.ppermute(values, axis, pairs)


def both(values, axis):
    size = lax.axis_size(axis)
    return pairwise(values, axis, size, True), pairwise(values, axis, size, False)


def call(kernel, outs, *operands, scratch=(), name):
    vmem = pl.BlockSpec(memory_space=pltpu.VMEM)
    held = [pltpu.with_memory_space_constraint(value, pltpu.VMEM) for value in operands]
    return pl.pallas_call(
        kernel,
        out_shape=outs,
        in_specs=[vmem] * len(held),
        out_specs=jax.tree.map(lambda _: vmem, outs),
        scratch_shapes=list(scratch),
        compiler_params=pltpu.CompilerParams(vmem_limit_bytes=VMEM_LIMIT),
        name=name,
    )(*held)


def is_even(axis):
    return lax.axis_index(axis) % 2 == 0


def ordered(odd_ref, even_ref, axis):
    even = is_even(axis)
    odd_pair, even_pair = odd_ref[...], even_ref[...]
    return jnp.where(even, odd_pair, even_pair), jnp.where(even, even_pair, odd_pair)


def shifted(values, c):
    if c == 0:
        return values
    return pltpu.roll(values, (-c) % values.shape[-1], values.ndim - 1)


def pack_kernel(u_ref, bone_ref, broken_ref, out_ref):
    out_ref[0:3] = u_ref[...]
    out_ref[3] = bone_ref[...].astype(F32)
    out_ref[4:8] = broken_ref[...].astype(F32)


def widen_kernel(own_ref, odd_ref, even_ref, out_ref):
    cells = own_ref.shape[1]
    low, high = ordered(odd_ref, even_ref, "gx")
    own = own_ref[...]
    for f in range(own.shape[0]):
        if f < 4:
            base = f * 3 * cells
            out_ref[base + 2 * cells : base + 3 * cells] = high[f]
        else:
            base = 12 * cells + (f - 4) * 2 * cells
        out_ref[base : base + cells] = low[f]
        out_ref[base + cells : base + 2 * cells] = own[f]


def stack_rows(own, low, high):
    return jnp.concatenate([low, own, high], axis=-2)


def fill_moving(u_refs, rolled_ref, own_ref, layers, cells, region):
    first, last = region
    own, low, high = u_refs
    for f in range(3):
        part = slice(f * layers, (f + 1) * layers)
        field = stack_rows(own[part], low[part], high[part])
        for c in range(-REACH, REACH + 1):
            rolled_ref[c + REACH, f] = shifted(field, c)
    for f in range(3):
        here = rolled_ref[REACH, f, cells : 2 * cells, first:last]
        for step in range(-REACH, REACH + 1):
            own_ref[f, step + REACH] = here - float(step)


def window(rolled_ref, c, f, a, b, cells, first, last):
    return rolled_ref[c + REACH, f, cells + a : 2 * cells + a, first + b : last + b]


def bond_pass(rolled_ref, own_ref, pen_of, along_ref, across_ref, cells, region, kinds):
    first, last = region
    shape = (cells, last - first, own_ref.shape[-1])
    totals = jnp.zeros(shape, F32)
    second = jnp.zeros(shape, F32)
    for squared, bonds in CLASSES.items():
        natural = math.sqrt(squared)
        moved = jnp.zeros(shape, F32)
        other = jnp.zeros(shape, F32)
        for a, b, c, word, bit, backward, place in bonds:
            rel = [
                window(rolled_ref, c, f, a, b, cells, first, last) - own_ref[f, step + REACH]
                for f, step in enumerate((a, b, c))
            ]
            square = rel[0] * rel[0] + rel[1] * rel[1] + rel[2] * rel[2]
            length = square * lax.rsqrt(jnp.maximum(square, 1e-30))
            scaled = (length - natural) * (HALF / natural)
            pen = pen_of(a, b, c, word, bit, backward, place)
            weight = 1.0 + jnp.tanh(pen - scaled)
            pulled = weight * scaled
            direction = lax.rsqrt(square + DIRECTION_EPS)
            along_ref[place] = weight * direction
            across_ref[place] = pulled * direction
            moved = moved + pulled
            other = other + (pen if kinds == "volume" else weight)
        totals = totals + moved * (0.5 * natural / HALF)
        if kinds == "volume":
            lost = (PEN * len(bonds) - other) * (1.0 / LOST)
            second = second + (len(bonds) - lost) * natural
        else:
            second = second + other * (0.5 * natural)
    return totals, second


def first_kernel(own_ref, odd_ref, even_ref, rolled_ref, pen_ref, along_ref, across_ref, ratio_ref, volume_ref, mine_ref, nb_ref, word_ref):
    rows = own_ref.shape[-2]
    depth = own_ref.shape[-1]
    cells = pen_ref.shape[1]
    layers = 3 * cells
    half = rows // 2
    region = (half, half + 2 * rows)
    low, high = ordered(odd_ref, even_ref, "gy")
    own = own_ref[...]
    fill_moving((own, low, high), rolled_ref, mine_ref, layers, cells, region)
    part = slice(3 * layers, 4 * layers)
    bone = stack_rows(own[part], low[part], high[part])
    void = jnp.where(bone == 0.0, -1, 0)
    lane = lax.broadcasted_iota(jnp.int32, void.shape, 2)
    for c in range(-REACH, REACH + 1):
        turned = shifted(void, c)
        if c != 0:
            turned = jnp.where((lane + c >= 0) & (lane + c < depth), turned, -1)
        nb_ref[c + REACH] = turned
    for w in range(4):
        part = slice(4 * layers + w * 2 * cells, 4 * layers + (w + 1) * 2 * cells)
        words = stack_rows(own[part], low[part], high[part]).astype(jnp.int32)
        for c in range(-REACH, REACH + 1):
            word_ref[c + REACH, w] = shifted(words, c) | nb_ref[c + REACH, 0 : 2 * cells]

    first, last = region

    def pen_of(a, b, c, word, bit, backward, place):
        if backward:
            words = word_ref[c + REACH, word, cells + a : 2 * cells + a, first + b : last + b]
            hit = words & (1 << bit)
        else:
            words = word_ref[REACH, word, cells : 2 * cells, first:last]
            far = nb_ref[c + REACH, cells + a : 2 * cells + a, first + b : last + b]
            hit = (words & (1 << bit)) | far
        pen = jnp.where(hit == 0, PEN, PEN - LOST)
        pen_ref[place] = pen
        return pen

    totals, volume = bond_pass(rolled_ref, mine_ref, pen_of, along_ref, across_ref, cells, region, "volume")
    solid = jnp.where(nb_ref[REACH, cells : 2 * cells, first:last] == 0, 1.0, 0.0)
    volume = jnp.maximum(volume * solid, 1.0)
    inverse = 1.0 / volume
    dilatation = 3.0 * (totals * solid) / volume
    ratio_ref[0] = dilatation * inverse * (0.5 * BULK_TERM)
    ratio_ref[1] = inverse * (0.5 * SHEAR_TERM / HALF)
    volume_ref[0] = volume
    volume_ref[1] = solid


def later_kernel(own_ref, odd_ref, even_ref, pen_ref, volume_ref, rolled_ref, along_ref, across_ref, ratio_ref, damage_ref, mine_ref):
    rows = own_ref.shape[-2]
    cells = pen_ref.shape[1]
    layers = 3 * cells
    half = rows // 2
    region = (half, half + 2 * rows)
    low, high = ordered(odd_ref, even_ref, "gy")
    fill_moving((own_ref[...], low, high), rolled_ref, mine_ref, layers, cells, region)

    def pen_of(a, b, c, word, bit, backward, place):
        return pen_ref[place]

    totals, held = bond_pass(rolled_ref, mine_ref, pen_of, along_ref, across_ref, cells, region, "weight")
    volume = volume_ref[0]
    solid = volume_ref[1]
    inverse = 1.0 / volume
    dilatation = 3.0 * (totals * solid) / volume
    ratio_ref[0] = dilatation * inverse * (0.5 * BULK_TERM)
    damage = 1.0 - (held * solid) / volume
    damage_ref[...] = damage[:, half : half + rows]


def forces(rolled_ref, along_ref, across_ref, scaled_ref, inverse_ref, cells, rows):
    half = rows // 2
    mine = slice(half, half + rows)
    layer = slice(cells, 2 * cells)
    total = [jnp.zeros((cells, rows, rolled_ref.shape[-1]), F32) for _ in range(3)]
    scaled = scaled_ref[REACH, layer, mine]
    inverse = inverse_ref[REACH, layer, mine]
    here = [rolled_ref[REACH, f, layer, rows : 2 * rows] for f in range(3)]
    for bonds in CLASSES.values():
        for a, b, c, word, bit, backward, place in bonds:
            far = (c + REACH, slice(cells + a, 2 * cells + a), slice(half + b, half + rows + b))
            magnitude = along_ref[place, :, mine] * (scaled + scaled_ref[far])
            magnitude = magnitude + across_ref[place, :, mine] * (inverse + inverse_ref[far])
            for f, step in enumerate((a, b, c)):
                rel = window(rolled_ref, c, f, a, b, cells, rows, 2 * rows) - here[f]
                if step:
                    rel = rel + float(step)
                total[f] = total[f] + magnitude * rel
    return total


def fill_ratio(target_ref, low, own, high):
    field = jnp.concatenate([low, own, high], axis=0)
    for c in range(-REACH, REACH + 1):
        target_ref[c + REACH] = shifted(field, c)


def move_kernel(rolled_ref, along_ref, across_ref, ratio_ref, odd_ref, even_ref, volume_ref, u_ref, v_ref, u_out, v_out, inverse_ref, scaled_ref):
    cells, rows = u_ref.shape[1], u_ref.shape[2]
    half = rows // 2
    low, high = ordered(odd_ref, even_ref, "gx")
    fill_ratio(scaled_ref, low[0], ratio_ref[0], high[0])
    fill_ratio(inverse_ref, low[1], ratio_ref[1], high[1])
    total = forces(rolled_ref, along_ref, across_ref, scaled_ref, inverse_ref, cells, rows)
    solid = volume_ref[1, :, half : half + rows]
    for f in range(3):
        speed = v_ref[f] + TIME_STEP * (total[f] * solid)
        v_out[f] = speed
        u_out[f] = u_ref[f] + TIME_STEP * speed


def last_kernel(rolled_ref, along_ref, across_ref, ratio_ref, odd_ref, even_ref, volume_ref, v_ref, inverse_ref, v_out, scaled_ref):
    cells, rows = v_ref.shape[1], v_ref.shape[2]
    half = rows // 2
    low, high = ordered(odd_ref, even_ref, "gx")
    fill_ratio(scaled_ref, low[0], ratio_ref[0], high[0])
    total = forces(rolled_ref, along_ref, across_ref, scaled_ref, inverse_ref, cells, rows)
    solid = volume_ref[1, :, half : half + rows]
    for f in range(3):
        v_out[f] = v_ref[f] + TIME_STEP * (total[f] * solid)


def widen_moving_kernel(own_ref, odd_ref, even_ref, out_ref):
    cells = own_ref.shape[1]
    low, high = ordered(odd_ref, even_ref, "gx")
    own = own_ref[...]
    for f in range(3):
        base = f * 3 * cells
        out_ref[base : base + cells] = low[f]
        out_ref[base + cells : base + 2 * cells] = own[f]
        out_ref[base + 2 * cells : base + 3 * cells] = high[f]


def body(displacement, velocity, bone, broken):
    cells, rows, depth = bone.shape
    if cells != REACH or rows != 8:
        raise ValueError("block size")
    layers, tall, region = 3 * cells, 3 * rows, 2 * rows
    turns = 2 * REACH + 1

    def vmem(*shape, dtype=F32):
        return pltpu.VMEM(shape, dtype)

    hbm = jax.ShapeDtypeStruct
    packed = call(pack_kernel, vmem(8, cells, rows, depth), displacement, bone, broken, name="pack")
    tiles = 4 * layers + 4 * 2 * cells
    wide = call(widen_kernel, vmem(tiles, rows, depth), packed, *both(packed, "gx"), name="widen")
    rolled, pen, along, across, ratio, volume = call(
        first_kernel,
        (
            vmem(turns, 3, layers, tall, depth),
            vmem(BONDS, cells, region, depth),
            vmem(BONDS, cells, region, depth),
            vmem(BONDS, cells, region, depth),
            vmem(2, cells, region, depth),
            vmem(2, cells, region, depth),
        ),
        wide,
        *both(wide, "gy"),
        scratch=(
            pltpu.VMEM((3, turns, cells, region, depth), F32),
            pltpu.VMEM((turns, layers, tall, depth), jnp.int32),
            pltpu.VMEM((turns, 4, 2 * cells, tall, depth), jnp.int32),
        ),
        name="first",
    )
    moved, speed, inverse = call(
        move_kernel,
        (
            vmem(3, cells, rows, depth),
            vmem(3, cells, rows, depth),
            vmem(turns, layers, region, depth),
        ),
        rolled,
        along,
        across,
        ratio,
        *both(ratio, "gx"),
        volume,
        displacement,
        velocity,
        scratch=(pltpu.VMEM((turns, layers, region, depth), F32),),
        name="move",
    )
    wide = call(widen_moving_kernel, vmem(3 * layers, rows, depth), moved, *both(moved, "gx"), name="widen_moving")
    rolled, along, across, ratio, damage = call(
        later_kernel,
        (
            vmem(turns, 3, layers, tall, depth),
            vmem(BONDS, cells, region, depth),
            vmem(BONDS, cells, region, depth),
            vmem(1, cells, region, depth),
            hbm((cells, rows, depth), F32),
        ),
        wide,
        *both(wide, "gy"),
        pen,
        volume,
        scratch=(pltpu.VMEM((3, turns, cells, region, depth), F32),),
        name="later",
    )
    speed = call(
        last_kernel,
        hbm((3, cells, rows, depth), F32),
        rolled,
        along,
        across,
        ratio,
        *both(ratio, "gx"),
        volume,
        speed,
        inverse,
        scratch=(pltpu.VMEM((turns, layers, region, depth), F32),),
        name="last",
    )
    return speed, damage


def solution(mesh):
    in_specs = (
        P(None, "gx", "gy", None),
        P(None, "gx", "gy", None),
        P("gx", "gy", None),
        P(None, "gx", "gy", None),
    )
    out_specs = (P(None, "gx", "gy", None), P("gx", "gy", None))
    return jax.shard_map(body, mesh=mesh, in_specs=in_specs, out_specs=out_specs, check_vma=False)
```

```python
import math

import jax
import jax.numpy as jnp
from jax import lax
from jax.experimental import pallas as pl
from jax.experimental.pallas import tpu as pltpu
from jax.sharding import PartitionSpec as P

BULK_TERM = -50.0
SHEAR_TERM = 1500.0
TIME_STEP = 0.1
STRETCH_CRITICAL = 0.04
STRETCH_WIDTH = 0.01
DIRECTION_EPS = 1e-06

REACH = 3
HALF = 0.5 / STRETCH_WIDTH
PEN = 0.5 * STRETCH_CRITICAL / STRETCH_WIDTH
LOST = 1024.0
F32 = jnp.float32
VMEM_LIMIT = 20 * 1024 * 1024


def half_bonds():
    listed = []
    for step_x in range(0, 4):
        for step_y in range(-3, 4):
            for step_z in range(-3, 4):
                forward_half = step_x > 0 or (
                    step_x == 0 and (step_y > 0 or (step_y == 0 and step_z > 0))
                )
                if forward_half and step_x * step_x + step_y * step_y + step_z * step_z <= 9:
                    listed.append((step_x, step_y, step_z))
    return listed


def flag_place(number):
    if number < 16:
        return (0, number)
    return (1 + (number - 16) // 15, (number - 16) % 15)


def bond_classes():
    classes = {}
    for number, (a, b, c) in enumerate(half_bonds()):
        word, bit = flag_place(number)
        group = classes.setdefault(a * a + b * b + c * c, [])
        group.append((a, b, c, word, bit, False))
        group.append((-a, -b, -c, word, bit, True))
    place = 0
    for squared in sorted(classes):
        classes[squared] = [bond + (place + k,) for k, bond in enumerate(classes[squared])]
        place += len(classes[squared])
    return {squared: classes[squared] for squared in sorted(classes)}, place


CLASSES, BONDS = bond_classes()


def pairwise(values, axis, odd):
    pairs = []
    for i in range(1 if odd else 0, lax.axis_size(axis) - 1, 2):
        pairs += [(i, i + 1), (i + 1, i)]
    return lax.ppermute(values, axis, pairs)


def both(odd_values, even_values, axis):
    return pairwise(odd_values, axis, True), pairwise(even_values, axis, False)


def call(kernel, outs, *operands, scratch=(), hbm=()):
    vmem = pl.BlockSpec(memory_space=pltpu.VMEM)
    spaces = [pltpu.HBM if n in hbm else pltpu.VMEM for n in range(len(operands))]
    held = [pltpu.with_memory_space_constraint(value, space) for value, space in zip(operands, spaces)]
    return pl.pallas_call(
        kernel,
        out_shape=outs,
        in_specs=[pl.BlockSpec(memory_space=space) for space in spaces],
        out_specs=jax.tree.map(lambda _: vmem, outs),
        scratch_shapes=list(scratch),
        compiler_params=pltpu.CompilerParams(vmem_limit_bytes=VMEM_LIMIT),
    )(*held)


def is_even(axis):
    return lax.axis_index(axis) % 2 == 0


def needed_rows(distance):
    return (6, 5, 5, 3)[distance]


def outer_rows(distance):
    return (3, 2, 2, 0)[distance]


def word_reach():
    reach = [0, 0, 0, 0]
    for number, (a, b, c) in enumerate(half_bonds()):
        word = flag_place(number)[0]
        reach[word] = max(reach[word], a)
    return reach


MOVING = [(f, x) for f in range(3) for x in range(3)]
SENT = MOVING + [(3, x) for x in range(3)]
SENT += [(4 + w, x) for w in range(4) for x in range(3 - word_reach()[w], 3)]
KEPT = [(4 + w, x) for w in range(4) for x in range(3) if (4 + w, x) not in SENT]


def strips(fields):
    placed, start = {}, 0
    for f in fields:
        for x in range(-3, 6):
            if f >= 4 and (x >= 3 or (x < 0 and (f, x + 3) not in SENT)):
                continue
            rows = needed_rows(max(0, -x, x - 2))
            placed[f, x] = (start, rows)
            start += rows
    return placed, start


ALL_STRIPS, ALL_ROWS = strips(range(8))
MOVING_STRIPS, MOVING_ROWS = strips(range(3))


def shifted(values, c):
    if c == 0:
        return values
    return pltpu.roll(values, (-c) % values.shape[-1], values.ndim - 1)


def pack_kernel(u_ref, bone_ref, broken_ref, sent_ref, kept_ref, bone_in, broken_in, sems):
    copies = [
        pltpu.make_async_copy(bone_ref, bone_in, sems.at[0]),
        pltpu.make_async_copy(broken_ref, broken_in, sems.at[1]),
    ]
    copies += [
        pltpu.make_async_copy(u_ref.at[f], sent_ref.at[3 * f : 3 * f + 3], sems.at[2 + f]) for f in range(3)
    ]
    for copy in copies:
        copy.start()
    copies[0].wait()
    sent_ref[9:12] = bone_in[...].astype(F32)
    copies[1].wait()
    for target, listed in ((sent_ref, SENT), (kept_ref, KEPT)):
        for n, (f, x) in enumerate(listed):
            if f >= 4:
                target[n] = broken_in[f - 4, x].astype(F32)
    for copy in copies[2:]:
        copy.wait()


def cut_strips(tile_of, placed, odd_ref, even_ref):
    even = is_even("gy")
    for (f, x), (start, rows) in placed.items():
        tile = tile_of(f, x)
        first, last = tile[0:rows], tile[tile.shape[0] - rows :]
        odd_ref[start : start + rows] = jnp.where(even, first, last)
        even_ref[start : start + rows] = jnp.where(even, last, first)


def widen_kernel(sent_ref, kept_ref, odd_ref, even_ref, side_ref, to_odd_ref, to_even_ref):
    even = is_even("gx")
    side_ref[0] = jnp.where(even, odd_ref[...], even_ref[...])
    side_ref[1] = jnp.where(even, even_ref[...], odd_ref[...])
    cut_strips(tiles(side_ref, sent_ref, kept_ref), ALL_STRIPS, to_odd_ref, to_even_ref)


def widen_moving_kernel(own_ref, odd_ref, even_ref, side_ref, to_odd_ref, to_even_ref):
    even = is_even("gx")
    side_ref[0] = jnp.where(even, odd_ref[...], even_ref[...])
    side_ref[1] = jnp.where(even, even_ref[...], odd_ref[...])
    cut_strips(tiles(side_ref, own_ref, None), MOVING_STRIPS, to_odd_ref, to_even_ref)


def tiles(side_ref, own_ref, kept_ref):
    def tile_of(f, x):
        if x < 0:
            return side_ref[0, SENT.index((f, x + 3))]
        if x >= 3:
            return side_ref[1, SENT.index((f, x - 3))]
        if (f, x) in KEPT:
            return kept_ref[KEPT.index((f, x))]
        return own_ref[SENT.index((f, x))]

    return tile_of


def lay(field_ref, f, tile_of, placed, odd_ref, even_ref):
    even = is_even("gy")
    rows = field_ref.shape[1] // 3
    field_ref[...] = jnp.zeros(field_ref.shape, F32)
    for x in range(-3, 6):
        if (f, x) in placed:
            start, count = placed[f, x]
            from_odd, from_even = odd_ref[start : start + count], even_ref[start : start + count]
            field_ref[x + 3, rows - count : rows] = jnp.where(even, from_odd, from_even)
            field_ref[x + 3, rows : 2 * rows] = tile_of(f, x)
            field_ref[x + 3, 2 * rows : 2 * rows + count] = jnp.where(even, from_even, from_odd)
    return field_ref[...]


def fill_moving(tile_of, placed, odd_ref, even_ref, field_ref, rolled_ref, own_ref, cells, region):
    first, last = region
    for f in range(3):
        field = lay(field_ref.at[f], f, tile_of, placed, odd_ref, even_ref)
        for c in range(-REACH, REACH + 1):
            rolled_ref[c + REACH, f] = shifted(field, c)
    for f in range(3):
        here = rolled_ref[REACH, f, cells : 2 * cells, first:last]
        for step in range(-REACH, REACH + 1):
            own_ref[f, step + REACH] = here - float(step)


def window(rolled_ref, c, f, a, b, cells, first, last):
    return rolled_ref[c + REACH, f, cells + a : 2 * cells + a, first + b : last + b]


def bond_pass(rolled_ref, own_ref, pen_of, along_ref, across_ref, cells, region, kinds):
    first, last = region
    shape = (cells, last - first, own_ref.shape[-1])
    totals = jnp.zeros(shape, F32)
    second = jnp.zeros(shape, F32)
    for squared, bonds in CLASSES.items():
        natural = math.sqrt(squared)
        moved = jnp.zeros(shape, F32)
        other = jnp.zeros(shape, F32)
        for a, b, c, word, bit, backward, place in bonds:
            rel = [
                window(rolled_ref, c, f, a, b, cells, first, last) - own_ref[f, step + REACH]
                for f, step in enumerate((a, b, c))
            ]
            square = rel[0] * rel[0] + rel[1] * rel[1] + rel[2] * rel[2]
            length = square * lax.rsqrt(jnp.maximum(square, 1e-30))
            scaled = (length - natural) * (HALF / natural)
            pen = pen_of(a, b, c, word, bit, backward, place)
            weight = 1.0 + jnp.tanh(pen - scaled)
            pulled = weight * scaled
            direction = lax.rsqrt(square + DIRECTION_EPS)
            along_ref[place] = weight * direction
            across_ref[place] = pulled * direction
            moved = moved + pulled
            other = other + (pen if kinds == "volume" else weight)
        totals = totals + moved * (0.5 * natural / HALF)
        if kinds == "volume":
            lost = (PEN * len(bonds) - other) * (1.0 / LOST)
            second = second + (len(bonds) - lost) * natural
        else:
            second = second + other * (0.5 * natural)
    return totals, second


def cut_ratio(ratio_ref, to_odd_ref, to_even_ref, rows):
    even = is_even("gx")
    half = rows // 2
    start = 0
    for f in range(ratio_ref.shape[0]):
        for distance in range(1, 4):
            count = rows + 2 * outer_rows(distance)
            part = slice(half - outer_rows(distance), half + rows + outer_rows(distance))
            upper = ratio_ref[f, 3 - distance, part]
            lower = ratio_ref[f, distance - 1, part]
            to_odd_ref[start : start + count] = jnp.where(even, lower, upper)
            to_even_ref[start : start + count] = jnp.where(even, upper, lower)
            start += count


def ratio_rows(rows):
    return sum(rows + 2 * outer_rows(distance) for distance in range(1, 4))


def first_kernel(side_ref, sent_ref, kept_ref, odd_ref, even_ref, v_hbm, rolled_ref, pen_ref, along_ref, across_ref, ratio_ref, to_odd_ref, to_even_ref, volume_ref, v_ref, mine_ref, field_ref, nb_ref, word_ref, sem):
    copy = pltpu.make_async_copy(v_hbm, v_ref, sem)
    copy.start()
    rows = sent_ref.shape[-2]
    depth = sent_ref.shape[-1]
    cells = pen_ref.shape[1]
    half = rows // 2
    region = (half, half + 2 * rows)
    tile_of = tiles(side_ref, sent_ref, kept_ref)
    fill_moving(tile_of, ALL_STRIPS, odd_ref, even_ref, field_ref, rolled_ref, mine_ref, cells, region)
    bone = lay(field_ref.at[0], 3, tile_of, ALL_STRIPS, odd_ref, even_ref)
    void = jnp.where(bone == 0.0, -1, 0)
    lane = lax.broadcasted_iota(jnp.int32, void.shape, 2)
    for c in range(-REACH, REACH + 1):
        turned = shifted(void, c)
        if c != 0:
            turned = jnp.where((lane + c >= 0) & (lane + c < depth), turned, -1)
        nb_ref[c + REACH] = turned
    for w in range(4):
        words = lay(field_ref.at[1 + w % 2], 4 + w, tile_of, ALL_STRIPS, odd_ref, even_ref)
        words = words[0 : 2 * cells].astype(jnp.int32)
        for c in range(-REACH, REACH + 1):
            word_ref[c + REACH, w] = shifted(words, c) | nb_ref[c + REACH, 0 : 2 * cells]

    first, last = region

    def pen_of(a, b, c, word, bit, backward, place):
        if backward:
            words = word_ref[c + REACH, word, cells + a : 2 * cells + a, first + b : last + b]
            hit = words & (1 << bit)
        else:
            words = word_ref[REACH, word, cells : 2 * cells, first:last]
            far = nb_ref[c + REACH, cells + a : 2 * cells + a, first + b : last + b]
            hit = (words & (1 << bit)) | far
        pen = jnp.where(hit == 0, PEN, PEN - LOST)
        pen_ref[place] = pen
        return pen

    totals, volume = bond_pass(rolled_ref, mine_ref, pen_of, along_ref, across_ref, cells, region, "volume")
    solid = jnp.where(nb_ref[REACH, cells : 2 * cells, first:last] == 0, 1.0, 0.0)
    volume = jnp.maximum(volume * solid, 1.0)
    inverse = 1.0 / volume
    dilatation = 3.0 * (totals * solid) / volume
    ratio_ref[0] = dilatation * inverse * (0.5 * BULK_TERM)
    ratio_ref[1] = inverse * (0.5 * SHEAR_TERM / HALF)
    cut_ratio(ratio_ref, to_odd_ref, to_even_ref, rows)
    volume_ref[0] = volume
    volume_ref[1] = solid
    copy.wait()


def later_kernel(side_ref, own_ref, odd_ref, even_ref, pen_ref, volume_ref, rolled_ref, along_ref, across_ref, ratio_ref, to_odd_ref, to_even_ref, damage_ref, mine_ref, field_ref):
    rows = own_ref.shape[-2]
    cells = pen_ref.shape[1]
    half = rows // 2
    region = (half, half + 2 * rows)
    tile_of = tiles(side_ref, own_ref, None)
    fill_moving(tile_of, MOVING_STRIPS, odd_ref, even_ref, field_ref, rolled_ref, mine_ref, cells, region)

    def pen_of(a, b, c, word, bit, backward, place):
        return pen_ref[place]

    totals, held = bond_pass(rolled_ref, mine_ref, pen_of, along_ref, across_ref, cells, region, "weight")
    volume = volume_ref[0]
    solid = volume_ref[1]
    inverse = 1.0 / volume
    dilatation = 3.0 * (totals * solid) / volume
    ratio_ref[0] = dilatation * inverse * (0.5 * BULK_TERM)
    cut_ratio(ratio_ref, to_odd_ref, to_even_ref, rows)
    damage = 1.0 - (held * solid) / volume
    damage_ref[...] = damage[:, half : half + rows]


def forces(total, inner, rolled_ref, along_ref, across_ref, scaled_ref, inverse_ref, rows):
    half = rows // 2
    mine = slice(half, half + rows)
    for x in range(3):
        scaled = scaled_ref[REACH, x + 3, mine]
        inverse = inverse_ref[REACH, x + 3, mine]
        here = [rolled_ref[REACH, f, x + 3, rows : 2 * rows] for f in range(3)]
        for bonds in CLASSES.values():
            for a, b, c, word, bit, backward, place in bonds:
                if (0 <= x + a < 3) != inner:
                    continue
                far = (c + REACH, x + 3 + a, slice(half + b, half + rows + b))
                magnitude = along_ref[place, x, mine] * (scaled + scaled_ref[far])
                magnitude = magnitude + across_ref[place, x, mine] * (inverse + inverse_ref[far])
                for f, step in enumerate((a, b, c)):
                    rel = rolled_ref[c + REACH, f, x + 3 + a, rows + b : 2 * rows + b] - here[f]
                    if step:
                        rel = rel + float(step)
                    total[f][x] = total[f][x] + magnitude * rel
    return total


def fill_inner(target_ref, own):
    for c in range(-REACH, REACH + 1):
        target_ref[c + REACH, 3:6] = shifted(own, c)


def fill_outer(target_ref, field_ref, f, odd_ref, even_ref, rows):
    even = is_even("gx")
    half = rows // 2
    field_ref[...] = jnp.zeros(field_ref.shape, F32)
    start = f * ratio_rows(rows)
    for distance in range(1, 4):
        count = rows + 2 * outer_rows(distance)
        part = slice(half - outer_rows(distance), half + rows + outer_rows(distance))
        from_odd, from_even = odd_ref[start : start + count], even_ref[start : start + count]
        field_ref[3 - distance, part] = jnp.where(even, from_odd, from_even)
        field_ref[2 + distance, part] = jnp.where(even, from_even, from_odd)
        start += count
    field = field_ref[...]
    for c in range(-REACH, REACH + 1):
        turned = shifted(field, c)
        target_ref[c + REACH, 0:3] = turned[0:3]
        target_ref[c + REACH, 6:9] = turned[3:6]


def start_total(rows, depth):
    return [[jnp.zeros((rows, depth), F32) for _ in range(3)] for _ in range(3)]


def inner_kernel(rolled_ref, along_ref, across_ref, ratio_ref, held_ref, part_ref, scaled_ref, inverse_ref):
    rows, depth = part_ref.shape[2:]
    fill_inner(scaled_ref, ratio_ref[0])
    if held_ref is None:
        held_ref = inverse_ref
        fill_inner(inverse_ref, ratio_ref[1])
    total = forces(start_total(rows, depth), True, rolled_ref, along_ref, across_ref, scaled_ref, held_ref, rows)
    for f in range(3):
        for x in range(3):
            part_ref[f, x] = total[f][x]


def first_inner_kernel(rolled_ref, along_ref, across_ref, ratio_ref, part_ref, scaled_ref, inverse_ref):
    inner_kernel(rolled_ref, along_ref, across_ref, ratio_ref, None, part_ref, scaled_ref, inverse_ref)


def last_inner_kernel(rolled_ref, along_ref, across_ref, ratio_ref, inverse_ref, part_ref, scaled_ref):
    inner_kernel(rolled_ref, along_ref, across_ref, ratio_ref, inverse_ref, part_ref, scaled_ref, None)


def outer_forces(rolled_ref, along_ref, across_ref, scaled_ref, inverse_ref, part_ref, rows):
    total = [[part_ref[f, x] for x in range(3)] for f in range(3)]
    return forces(total, False, rolled_ref, along_ref, across_ref, scaled_ref, inverse_ref, rows)


def move_kernel(rolled_ref, along_ref, across_ref, ratio_ref, part_ref, odd_ref, even_ref, volume_ref, sent_ref, v_ref, u_out, v_out, inverse_ref, scaled_ref, field_ref):
    rows = v_ref.shape[2]
    half = rows // 2
    for f, target in ((0, scaled_ref), (1, inverse_ref)):
        fill_outer(target, field_ref.at[f], f, odd_ref, even_ref, rows)
        fill_inner(target, ratio_ref[f])
    total = outer_forces(rolled_ref, along_ref, across_ref, scaled_ref, inverse_ref, part_ref, rows)
    for f in range(3):
        for x in range(3):
            speed = v_ref[f, x] + TIME_STEP * (total[f][x] * volume_ref[1, x, half : half + rows])
            v_out[f, x] = speed
            u_out[3 * f + x] = sent_ref[3 * f + x] + TIME_STEP * speed


def last_kernel(rolled_ref, along_ref, across_ref, ratio_ref, part_ref, odd_ref, even_ref, volume_ref, v_ref, inverse_ref, damage_ref, v_out, damage_out, scaled_ref, field_ref):
    rows = v_ref.shape[2]
    half = rows // 2
    damage_out[...] = damage_ref[...]
    fill_outer(scaled_ref, field_ref, 0, odd_ref, even_ref, rows)
    scaled_ref[REACH, 3:6] = ratio_ref[0]
    total = outer_forces(rolled_ref, along_ref, across_ref, scaled_ref, inverse_ref, part_ref, rows)
    for f in range(3):
        for x in range(3):
            v_out[f, x] = v_ref[f, x] + TIME_STEP * (total[f][x] * volume_ref[1, x, half : half + rows])


def body(displacement, velocity, bone, broken):
    cells, rows, depth = bone.shape
    if cells != REACH or rows != 8:
        raise ValueError("block size")
    layers, tall, region = 3 * cells, 3 * rows, 2 * rows
    turns = 2 * REACH + 1

    def vmem(*shape, dtype=F32):
        return pltpu.VMEM(shape, dtype)

    hbm = jax.ShapeDtypeStruct
    sent, kept = call(
        pack_kernel,
        (vmem(len(SENT), rows, depth), vmem(len(KEPT), rows, depth)),
        displacement,
        bone,
        broken,
        scratch=(
            vmem(cells, rows, depth, dtype=jnp.int32),
            vmem(4, cells, rows, depth, dtype=jnp.int32),
            pltpu.SemaphoreType.DMA((5,)),
        ),
        hbm=(0, 1, 2),
    )
    side, to_odd, to_even = call(
        widen_kernel,
        (vmem(2, len(SENT), rows, depth), vmem(ALL_ROWS, depth), vmem(ALL_ROWS, depth)),
        sent,
        kept,
        *both(sent, sent, "gx"),
    )
    bonds = (BONDS, cells, region, depth)
    crossing = ratio_rows(rows)
    rolled, pen, along, across, ratio, to_odd, to_even, volume, speed = call(
        first_kernel,
        (
            vmem(turns, 3, layers, tall, depth),
            vmem(*bonds),
            vmem(*bonds),
            vmem(*bonds),
            vmem(2, cells, region, depth),
            vmem(2 * crossing, depth),
            vmem(2 * crossing, depth),
            vmem(2, cells, region, depth),
            vmem(3, cells, rows, depth),
        ),
        side,
        sent,
        kept,
        *both(to_odd, to_even, "gy"),
        velocity,
        scratch=(
            vmem(3, turns, cells, region, depth),
            vmem(3, layers, tall, depth),
            vmem(turns, layers, tall, depth, dtype=jnp.int32),
            vmem(turns, 4, 2 * cells, tall, depth, dtype=jnp.int32),
            pltpu.SemaphoreType.DMA(()),
        ),
        hbm=(5,),
    )
    arrived = both(to_odd, to_even, "gx")
    wide_ratio = vmem(turns, layers, region, depth)
    part = call(
        first_inner_kernel, vmem(3, cells, rows, depth), rolled, along, across, ratio, scratch=(wide_ratio, wide_ratio)
    )
    moved, speed, inverse = call(
        move_kernel,
        (vmem(3 * cells, rows, depth), vmem(3, cells, rows, depth), wide_ratio),
        rolled,
        along,
        across,
        ratio,
        part,
        *arrived,
        volume,
        sent,
        speed,
        scratch=(wide_ratio, vmem(2, 6, region, depth)),
    )
    side, to_odd, to_even = call(
        widen_moving_kernel,
        (vmem(2, len(MOVING), rows, depth), vmem(MOVING_ROWS, depth), vmem(MOVING_ROWS, depth)),
        moved,
        *both(moved, moved, "gx"),
    )
    rolled, along, across, ratio, to_odd, to_even, damage = call(
        later_kernel,
        (
            vmem(turns, 3, layers, tall, depth),
            vmem(*bonds),
            vmem(*bonds),
            vmem(1, cells, region, depth),
            vmem(crossing, depth),
            vmem(crossing, depth),
            vmem(cells, rows, depth),
        ),
        side,
        moved,
        *both(to_odd, to_even, "gy"),
        pen,
        volume,
        scratch=(
            vmem(3, turns, cells, region, depth),
            vmem(3, layers, tall, depth),
        ),
    )
    arrived = both(to_odd, to_even, "gx")
    part = call(
        last_inner_kernel, vmem(3, cells, rows, depth), rolled, along, across, ratio, inverse, scratch=(wide_ratio,)
    )
    return call(
        last_kernel,
        (hbm((3, cells, rows, depth), F32), hbm((cells, rows, depth), F32)),
        rolled,
        along,
        across,
        ratio,
        part,
        *arrived,
        volume,
        speed,
        inverse,
        damage,
        scratch=(wide_ratio, vmem(6, region, depth)),
    )


def solution(mesh):
    in_specs = (
        P(None, "gx", "gy", None),
        P(None, "gx", "gy", None),
        P("gx", "gy", None),
        P(None, "gx", "gy", None),
    )
    out_specs = (P(None, "gx", "gy", None), P("gx", "gy", None))
    return jax.shard_map(body, mesh=mesh, in_specs=in_specs, out_specs=out_specs, check_vma=False)
```

```python
import math

import jax
import jax.numpy as jnp
from jax import lax
from jax.experimental import pallas as pl
from jax.experimental.pallas import tpu as pltpu
from jax.sharding import PartitionSpec as P

BULK_TERM = -50.0
SHEAR_TERM = 1500.0
TIME_STEP = 0.1
STRETCH_CRITICAL = 0.04
STRETCH_WIDTH = 0.01
DIRECTION_EPS = 1e-06

REACH = 3
HALF = 0.5 / STRETCH_WIDTH
PEN = 0.5 * STRETCH_CRITICAL / STRETCH_WIDTH
LOST = 1024.0
F32 = jnp.float32
VMEM_LIMIT = 20 * 1024 * 1024


def half_bonds():
    listed = []
    for step_x in range(0, 4):
        for step_y in range(-3, 4):
            for step_z in range(-3, 4):
                forward_half = step_x > 0 or (
                    step_x == 0 and (step_y > 0 or (step_y == 0 and step_z > 0))
                )
                if forward_half and step_x * step_x + step_y * step_y + step_z * step_z <= 9:
                    listed.append((step_x, step_y, step_z))
    return listed


def flag_place(number):
    if number < 16:
        return (0, number)
    return (1 + (number - 16) // 15, (number - 16) % 15)


def bond_classes():
    classes = {}
    for number, (a, b, c) in enumerate(half_bonds()):
        word, bit = flag_place(number)
        group = classes.setdefault(a * a + b * b + c * c, [])
        group.append((a, b, c, word, bit, False))
        group.append((-a, -b, -c, word, bit, True))
    place = 0
    for squared in sorted(classes):
        classes[squared] = [bond + (place + k,) for k, bond in enumerate(classes[squared])]
        place += len(classes[squared])
    return {squared: classes[squared] for squared in sorted(classes)}, place


CLASSES, BONDS = bond_classes()
DIRECTED = [bond for bonds in CLASSES.values() for bond in bonds]


def layers_read(c, word=None):
    reach = [
        a for a, b, step, held, bit, backward, place in DIRECTED
        if step == c and (word is None or (backward and held == word))
    ]
    if c == 0:
        reach.append(0)
    return slice(3 + min(reach), 6 + max(reach)) if reach else None


def pairwise(values, axis, odd):
    pairs = []
    for i in range(1 if odd else 0, lax.axis_size(axis) - 1, 2):
        pairs += [(i, i + 1), (i + 1, i)]
    return lax.ppermute(values, axis, pairs)


def both(odd_values, even_values, axis):
    return pairwise(odd_values, axis, True), pairwise(even_values, axis, False)


def call(kernel, outs, *operands, scratch=(), hbm=()):
    vmem = pl.BlockSpec(memory_space=pltpu.VMEM)
    spaces = [pltpu.HBM if n in hbm else pltpu.VMEM for n in range(len(operands))]
    held = [pltpu.with_memory_space_constraint(value, space) for value, space in zip(operands, spaces)]
    return pl.pallas_call(
        kernel,
        out_shape=outs,
        in_specs=[pl.BlockSpec(memory_space=space) for space in spaces],
        out_specs=jax.tree.map(lambda _: vmem, outs),
        scratch_shapes=list(scratch),
        compiler_params=pltpu.CompilerParams(vmem_limit_bytes=VMEM_LIMIT),
    )(*held)


def is_even(axis):
    return lax.axis_index(axis) % 2 == 0


def needed_rows(distance):
    return (6, 5, 5, 3)[distance]


def outer_rows(distance):
    return (3, 2, 2, 0)[distance]


def word_reach():
    reach = [0, 0, 0, 0]
    for number, (a, b, c) in enumerate(half_bonds()):
        word = flag_place(number)[0]
        reach[word] = max(reach[word], a)
    return reach


MOVING = [(f, x) for f in range(3) for x in range(3)]
SENT = MOVING + [(3, x) for x in range(3)]
SENT += [(4 + w, x) for w in range(4) for x in range(3 - word_reach()[w], 3)]
KEPT = [(4 + w, x) for w in range(4) for x in range(3) if (4 + w, x) not in SENT]


def strips(fields):
    placed, start = {}, 0
    for f in fields:
        for x in range(-3, 6):
            if f >= 4 and (x >= 3 or (x < 0 and (f, x + 3) not in SENT)):
                continue
            rows = needed_rows(max(0, -x, x - 2))
            placed[f, x] = (start, rows)
            start += rows
    return placed, start


ALL_STRIPS, ALL_ROWS = strips(range(8))
MOVING_STRIPS, MOVING_ROWS = strips(range(3))


def shifted(values, c):
    if c == 0:
        return values
    return pltpu.roll(values, (-c) % values.shape[-1], values.ndim - 1)


def pack_kernel(u_ref, bone_ref, broken_ref, sent_ref, kept_ref, bone_in, broken_in, sems):
    copies = [
        pltpu.make_async_copy(bone_ref, bone_in, sems.at[0]),
        pltpu.make_async_copy(broken_ref, broken_in, sems.at[1]),
    ]
    copies += [
        pltpu.make_async_copy(u_ref.at[f], sent_ref.at[3 * f : 3 * f + 3], sems.at[2 + f]) for f in range(3)
    ]
    for copy in copies:
        copy.start()
    copies[0].wait()
    sent_ref[9:12] = bone_in[...].astype(F32)
    copies[1].wait()
    for target, listed in ((sent_ref, SENT), (kept_ref, KEPT)):
        for n, (f, x) in enumerate(listed):
            if f >= 4:
                target[n] = broken_in[f - 4, x].astype(F32)
    for copy in copies[2:]:
        copy.wait()


def cut_strips(tile_of, placed, odd_ref, even_ref):
    even = is_even("gy")
    for (f, x), (start, rows) in placed.items():
        tile = tile_of(f, x)
        first, last = tile[0:rows], tile[tile.shape[0] - rows :]
        odd_ref[start : start + rows] = jnp.where(even, first, last)
        even_ref[start : start + rows] = jnp.where(even, last, first)


def widen_kernel(sent_ref, kept_ref, odd_ref, even_ref, side_ref, to_odd_ref, to_even_ref):
    even = is_even("gx")
    side_ref[0] = jnp.where(even, odd_ref[...], even_ref[...])
    side_ref[1] = jnp.where(even, even_ref[...], odd_ref[...])
    cut_strips(tiles(side_ref, sent_ref, kept_ref), ALL_STRIPS, to_odd_ref, to_even_ref)


def widen_moving_kernel(own_ref, odd_ref, even_ref, side_ref, to_odd_ref, to_even_ref):
    even = is_even("gx")
    side_ref[0] = jnp.where(even, odd_ref[...], even_ref[...])
    side_ref[1] = jnp.where(even, even_ref[...], odd_ref[...])
    cut_strips(tiles(side_ref, own_ref, None), MOVING_STRIPS, to_odd_ref, to_even_ref)


def tiles(side_ref, own_ref, kept_ref):
    def tile_of(f, x):
        if x < 0:
            return side_ref[0, SENT.index((f, x + 3))]
        if x >= 3:
            return side_ref[1, SENT.index((f, x - 3))]
        if (f, x) in KEPT:
            return kept_ref[KEPT.index((f, x))]
        return own_ref[SENT.index((f, x))]

    return tile_of


def lay(field_ref, f, tile_of, placed, odd_ref, even_ref):
    even = is_even("gy")
    rows = field_ref.shape[1] // 3
    for x in range(-3, 6):
        if (f, x) in placed:
            field_ref[x + 3, 0:rows] = jnp.zeros((rows, field_ref.shape[2]), F32)
            field_ref[x + 3, 2 * rows : 3 * rows] = jnp.zeros((rows, field_ref.shape[2]), F32)
            start, count = placed[f, x]
            from_odd, from_even = odd_ref[start : start + count], even_ref[start : start + count]
            field_ref[x + 3, rows - count : rows] = jnp.where(even, from_odd, from_even)
            field_ref[x + 3, rows : 2 * rows] = tile_of(f, x)
            field_ref[x + 3, 2 * rows : 2 * rows + count] = jnp.where(even, from_even, from_odd)
    return field_ref[...]


def fill_moving(tile_of, placed, odd_ref, even_ref, field_ref, rolled_ref, own_ref, cells, region):
    first, last = region
    for f in range(3):
        field = lay(field_ref.at[f], f, tile_of, placed, odd_ref, even_ref)
        for c in range(-REACH, REACH + 1):
            part = layers_read(c)
            rolled_ref[c + REACH, f, part] = shifted(field[part], c)
    for f in range(3):
        here = rolled_ref[REACH, f, cells : 2 * cells, first:last]
        for step in range(-REACH, REACH + 1):
            own_ref[f, step + REACH] = here - float(step)


def bond_pass(rolled_ref, own_ref, pen_of, square_ref, along_ref, across_ref, out_ref, region, kinds):
    first, last = region
    shape = (last - first, own_ref.shape[-1])

    def layer(x, carry):
        totals = jnp.zeros(shape, F32)
        second = jnp.zeros(shape, F32)
        for squared, bonds in CLASSES.items():
            natural = math.sqrt(squared)
            moved = jnp.zeros(shape, F32)
            other = jnp.zeros(shape, F32)
            for a, b, c, word, bit, backward, place in bonds:
                rel = [
                    rolled_ref[c + REACH, f, x + 3 + a, first + b : last + b] - own_ref[f, step + REACH, x]
                    for f, step in enumerate((a, b, c))
                ]
                square = rel[0] * rel[0] + rel[1] * rel[1] + rel[2] * rel[2]
                length = square * lax.rsqrt(jnp.maximum(square, 1e-30))
                scaled = (length - natural) * (HALF / natural)
                pen = pen_of(a, b, c, word, bit, backward, place, x)
                weight = 1.0 + jnp.tanh(pen - scaled)
                pulled = weight * scaled
                square_ref[place, x] = square
                along_ref[place, x] = weight
                across_ref[place, x] = pulled
                moved = moved + pulled
                other = other + (pen if kinds == "volume" else weight)
            totals = totals + moved * (0.5 * natural / HALF)
            if kinds == "volume":
                lost = (PEN * len(bonds) - other) * (1.0 / LOST)
                second = second + (len(bonds) - lost) * natural
            else:
                second = second + other * (0.5 * natural)
        out_ref[0, x] = totals
        out_ref[1, x] = second
        return carry

    lax.fori_loop(0, 3, layer, 0)
    return out_ref[0], out_ref[1]


def cut_ratio(ratio_ref, to_odd_ref, to_even_ref, rows):
    even = is_even("gx")
    half = rows // 2
    start = 0
    for f in range(ratio_ref.shape[0]):
        for distance in range(1, 4):
            count = rows + 2 * outer_rows(distance)
            part = slice(half - outer_rows(distance), half + rows + outer_rows(distance))
            upper = ratio_ref[f, 3 - distance, part]
            lower = ratio_ref[f, distance - 1, part]
            to_odd_ref[start : start + count] = jnp.where(even, lower, upper)
            to_even_ref[start : start + count] = jnp.where(even, upper, lower)
            start += count


def ratio_rows(rows):
    return sum(rows + 2 * outer_rows(distance) for distance in range(1, 4))


def first_kernel(side_ref, sent_ref, kept_ref, odd_ref, even_ref, v_hbm, rolled_ref, pen_ref, square_ref, along_ref, across_ref, ratio_ref, to_odd_ref, to_even_ref, volume_ref, v_ref, mine_ref, field_ref, nb_ref, word_ref, sums_ref, sem):
    copy = pltpu.make_async_copy(v_hbm, v_ref, sem)
    copy.start()
    rows = sent_ref.shape[-2]
    depth = sent_ref.shape[-1]
    cells = pen_ref.shape[1]
    half = rows // 2
    region = (half, half + 2 * rows)
    tile_of = tiles(side_ref, sent_ref, kept_ref)
    fill_moving(tile_of, ALL_STRIPS, odd_ref, even_ref, field_ref, rolled_ref, mine_ref, cells, region)
    bone = lay(field_ref.at[0], 3, tile_of, ALL_STRIPS, odd_ref, even_ref)
    void = jnp.where(bone == 0.0, -1, 0)
    for c in range(-REACH, REACH + 1):
        part = layers_read(c)
        turned = shifted(void[part], c)
        if c != 0:
            lane = lax.broadcasted_iota(jnp.int32, turned.shape, 2) + c
            turned = jnp.where((lane >= 0) & (lane < depth), turned, -1)
        nb_ref[c + REACH, part] = turned
    for w in range(4):
        words = lay(field_ref.at[1 + w % 2], 4 + w, tile_of, ALL_STRIPS, odd_ref, even_ref)
        words = words[0 : 2 * cells].astype(jnp.int32)
        for c in range(-REACH, REACH + 1):
            part = layers_read(c, w)
            if part is not None:
                word_ref[c + REACH, w, part] = shifted(words[part], c) | nb_ref[c + REACH, part]

    first, last = region

    def pen_of(a, b, c, word, bit, backward, place, x):
        if backward:
            words = word_ref[c + REACH, word, x + 3 + a, first + b : last + b]
            hit = words & (1 << bit)
        else:
            words = word_ref[REACH, word, x + 3, first:last]
            far = nb_ref[c + REACH, x + 3 + a, first + b : last + b]
            hit = (words & (1 << bit)) | far
        pen = jnp.where(hit == 0, PEN, PEN - LOST)
        pen_ref[place, x] = pen
        return pen

    totals, volume = bond_pass(rolled_ref, mine_ref, pen_of, square_ref, along_ref, across_ref, sums_ref, region, "volume")
    solid = jnp.where(nb_ref[REACH, cells : 2 * cells, first:last] == 0, 1.0, 0.0)
    volume = jnp.maximum(volume * solid, 1.0)
    inverse = 1.0 / volume
    dilatation = 3.0 * (totals * solid) / volume
    ratio_ref[0] = dilatation * inverse * (0.5 * BULK_TERM)
    ratio_ref[1] = inverse * (0.5 * SHEAR_TERM / HALF)
    cut_ratio(ratio_ref, to_odd_ref, to_even_ref, rows)
    volume_ref[0] = volume
    volume_ref[1] = solid
    copy.wait()


def later_kernel(side_ref, own_ref, odd_ref, even_ref, pen_ref, volume_ref, rolled_ref, square_ref, along_ref, across_ref, ratio_ref, to_odd_ref, to_even_ref, damage_ref, mine_ref, field_ref, sums_ref):
    rows = own_ref.shape[-2]
    cells = pen_ref.shape[1]
    half = rows // 2
    region = (half, half + 2 * rows)
    tile_of = tiles(side_ref, own_ref, None)
    fill_moving(tile_of, MOVING_STRIPS, odd_ref, even_ref, field_ref, rolled_ref, mine_ref, cells, region)

    def pen_of(a, b, c, word, bit, backward, place, x):
        return pen_ref[place, x]

    totals, held = bond_pass(rolled_ref, mine_ref, pen_of, square_ref, along_ref, across_ref, sums_ref, region, "weight")
    volume = volume_ref[0]
    solid = volume_ref[1]
    inverse = 1.0 / volume
    dilatation = 3.0 * (totals * solid) / volume
    ratio_ref[0] = dilatation * inverse * (0.5 * BULK_TERM)
    cut_ratio(ratio_ref, to_odd_ref, to_even_ref, rows)
    damage = 1.0 - (held * solid) / volume
    damage_ref[...] = damage[:, half : half + rows]


def forces(total, inner, rolled_ref, square_ref, along_ref, across_ref, scaled_ref, inverse_ref, rows):
    half = rows // 2
    mine = slice(half, half + rows)
    for x in range(3):
        scaled = scaled_ref[REACH, x + 3, mine]
        inverse = inverse_ref[REACH, x + 3, mine]
        here = [rolled_ref[REACH, f, x + 3, rows : 2 * rows] for f in range(3)]
        for bonds in CLASSES.values():
            for a, b, c, word, bit, backward, place in bonds:
                if (0 <= x + a < 3) != inner:
                    continue
                far = (c + REACH, x + 3 + a, slice(half + b, half + rows + b))
                magnitude = along_ref[place, x, mine] * (scaled + scaled_ref[far])
                magnitude = magnitude + across_ref[place, x, mine] * (inverse + inverse_ref[far])
                magnitude = magnitude * lax.rsqrt(square_ref[place, x, mine] + DIRECTION_EPS)
                for f, step in enumerate((a, b, c)):
                    rel = rolled_ref[c + REACH, f, x + 3 + a, rows + b : 2 * rows + b] - here[f]
                    if step:
                        rel = rel + float(step)
                    total[f][x] = total[f][x] + magnitude * rel
    return total


def fill_inner(target_ref, own):
    for c in range(-REACH, REACH + 1):
        target_ref[c + REACH, 3:6] = shifted(own, c)


def fill_outer(target_ref, field_ref, f, odd_ref, even_ref, rows):
    even = is_even("gx")
    half = rows // 2
    field_ref[...] = jnp.zeros(field_ref.shape, F32)
    start = f * ratio_rows(rows)
    for distance in range(1, 4):
        count = rows + 2 * outer_rows(distance)
        part = slice(half - outer_rows(distance), half + rows + outer_rows(distance))
        from_odd, from_even = odd_ref[start : start + count], even_ref[start : start + count]
        field_ref[3 - distance, part] = jnp.where(even, from_odd, from_even)
        field_ref[2 + distance, part] = jnp.where(even, from_even, from_odd)
        start += count
    field = field_ref[...]
    for c in range(-REACH, REACH + 1):
        turned = shifted(field, c)
        target_ref[c + REACH, 0:3] = turned[0:3]
        target_ref[c + REACH, 6:9] = turned[3:6]


def start_total(rows, depth):
    return [[jnp.zeros((rows, depth), F32) for _ in range(3)] for _ in range(3)]


def inner_kernel(rolled_ref, square_ref, along_ref, across_ref, ratio_ref, held_ref, part_ref, scaled_ref, inverse_ref):
    rows, depth = part_ref.shape[2:]
    fill_inner(scaled_ref, ratio_ref[0])
    if held_ref is None:
        held_ref = inverse_ref
        fill_inner(inverse_ref, ratio_ref[1])
    total = forces(start_total(rows, depth), True, rolled_ref, square_ref, along_ref, across_ref, scaled_ref, held_ref, rows)
    for f in range(3):
        for x in range(3):
            part_ref[f, x] = total[f][x]


def first_inner_kernel(rolled_ref, square_ref, along_ref, across_ref, ratio_ref, part_ref, scaled_ref, inverse_ref):
    inner_kernel(rolled_ref, square_ref, along_ref, across_ref, ratio_ref, None, part_ref, scaled_ref, inverse_ref)


def last_inner_kernel(rolled_ref, square_ref, along_ref, across_ref, ratio_ref, inverse_ref, part_ref, scaled_ref):
    inner_kernel(rolled_ref, square_ref, along_ref, across_ref, ratio_ref, inverse_ref, part_ref, scaled_ref, None)


def outer_forces(rolled_ref, square_ref, along_ref, across_ref, scaled_ref, inverse_ref, part_ref, rows):
    total = [[part_ref[f, x] for x in range(3)] for f in range(3)]
    return forces(total, False, rolled_ref, square_ref, along_ref, across_ref, scaled_ref, inverse_ref, rows)


def move_kernel(rolled_ref, square_ref, along_ref, across_ref, ratio_ref, part_ref, odd_ref, even_ref, volume_ref, sent_ref, v_ref, u_out, v_out, inverse_ref, scaled_ref, field_ref):
    rows = v_ref.shape[2]
    half = rows // 2
    for f, target in ((0, scaled_ref), (1, inverse_ref)):
        fill_outer(target, field_ref.at[f], f, odd_ref, even_ref, rows)
        fill_inner(target, ratio_ref[f])
    total = outer_forces(rolled_ref, square_ref, along_ref, across_ref, scaled_ref, inverse_ref, part_ref, rows)
    for f in range(3):
        for x in range(3):
            speed = v_ref[f, x] + TIME_STEP * (total[f][x] * volume_ref[1, x, half : half + rows])
            v_out[f, x] = speed
            u_out[3 * f + x] = sent_ref[3 * f + x] + TIME_STEP * speed


def last_kernel(rolled_ref, square_ref, along_ref, across_ref, ratio_ref, part_ref, odd_ref, even_ref, volume_ref, v_ref, inverse_ref, damage_ref, v_out, damage_out, scaled_ref, field_ref):
    rows = v_ref.shape[2]
    half = rows // 2
    damage_out[...] = damage_ref[...]
    fill_outer(scaled_ref, field_ref, 0, odd_ref, even_ref, rows)
    scaled_ref[REACH, 3:6] = ratio_ref[0]
    total = outer_forces(rolled_ref, square_ref, along_ref, across_ref, scaled_ref, inverse_ref, part_ref, rows)
    for f in range(3):
        for x in range(3):
            v_out[f, x] = v_ref[f, x] + TIME_STEP * (total[f][x] * volume_ref[1, x, half : half + rows])


def body(displacement, velocity, bone, broken):
    cells, rows, depth = bone.shape
    if cells != REACH or rows != 8:
        raise ValueError("block size")
    layers, tall, region = 3 * cells, 3 * rows, 2 * rows
    turns = 2 * REACH + 1

    def vmem(*shape, dtype=F32):
        return pltpu.VMEM(shape, dtype)

    hbm = jax.ShapeDtypeStruct
    sent, kept = call(
        pack_kernel,
        (vmem(len(SENT), rows, depth), vmem(len(KEPT), rows, depth)),
        displacement,
        bone,
        broken,
        scratch=(
            vmem(cells, rows, depth, dtype=jnp.int32),
            vmem(4, cells, rows, depth, dtype=jnp.int32),
            pltpu.SemaphoreType.DMA((5,)),
        ),
        hbm=(0, 1, 2),
    )
    side, to_odd, to_even = call(
        widen_kernel,
        (vmem(2, len(SENT), rows, depth), vmem(ALL_ROWS, depth), vmem(ALL_ROWS, depth)),
        sent,
        kept,
        *both(sent, sent, "gx"),
    )
    bonds = (BONDS, cells, region, depth)
    crossing = ratio_rows(rows)
    rolled, pen, square, along, across, ratio, to_odd, to_even, volume, speed = call(
        first_kernel,
        (
            vmem(turns, 3, layers, tall, depth),
            vmem(*bonds),
            vmem(*bonds),
            vmem(*bonds),
            vmem(*bonds),
            vmem(2, cells, region, depth),
            vmem(2 * crossing, depth),
            vmem(2 * crossing, depth),
            vmem(2, cells, region, depth),
            vmem(3, cells, rows, depth),
        ),
        side,
        sent,
        kept,
        *both(to_odd, to_even, "gy"),
        velocity,
        scratch=(
            vmem(3, turns, cells, region, depth),
            vmem(3, layers, tall, depth),
            vmem(turns, layers, tall, depth, dtype=jnp.int32),
            vmem(turns, 4, 2 * cells, tall, depth, dtype=jnp.int32),
            vmem(2, cells, region, depth),
            pltpu.SemaphoreType.DMA(()),
        ),
        hbm=(5,),
    )
    arrived = both(to_odd, to_even, "gx")
    wide_ratio = vmem(turns, layers, region, depth)
    part = call(
        first_inner_kernel,
        vmem(3, cells, rows, depth),
        rolled,
        square,
        along,
        across,
        ratio,
        scratch=(wide_ratio, wide_ratio),
    )
    moved, speed, inverse = call(
        move_kernel,
        (vmem(3 * cells, rows, depth), vmem(3, cells, rows, depth), wide_ratio),
        rolled,
        square,
        along,
        across,
        ratio,
        part,
        *arrived,
        volume,
        sent,
        speed,
        scratch=(wide_ratio, vmem(2, 6, region, depth)),
    )
    side, to_odd, to_even = call(
        widen_moving_kernel,
        (vmem(2, len(MOVING), rows, depth), vmem(MOVING_ROWS, depth), vmem(MOVING_ROWS, depth)),
        moved,
        *both(moved, moved, "gx"),
    )
    rolled, square, along, across, ratio, to_odd, to_even, damage = call(
        later_kernel,
        (
            vmem(turns, 3, layers, tall, depth),
            vmem(*bonds),
            vmem(*bonds),
            vmem(*bonds),
            vmem(1, cells, region, depth),
            vmem(crossing, depth),
            vmem(crossing, depth),
            vmem(cells, rows, depth),
        ),
        side,
        moved,
        *both(to_odd, to_even, "gy"),
        pen,
        volume,
        scratch=(
            vmem(3, turns, cells, region, depth),
            vmem(3, layers, tall, depth),
            vmem(2, cells, region, depth),
        ),
    )
    arrived = both(to_odd, to_even, "gx")
    part = call(
        last_inner_kernel,
        vmem(3, cells, rows, depth),
        rolled,
        square,
        along,
        across,
        ratio,
        inverse,
        scratch=(wide_ratio,),
    )
    return call(
        last_kernel,
        (hbm((3, cells, rows, depth), F32), hbm((cells, rows, depth), F32)),
        rolled,
        square,
        along,
        across,
        ratio,
        part,
        *arrived,
        volume,
        speed,
        inverse,
        damage,
        scratch=(wide_ratio, vmem(6, region, depth)),
    )


def solution(mesh):
    in_specs = (
        P(None, "gx", "gy", None),
        P(None, "gx", "gy", None),
        P("gx", "gy", None),
        P(None, "gx", "gy", None),
    )
    out_specs = (P(None, "gx", "gy", None), P("gx", "gy", None))
    return jax.shard_map(body, mesh=mesh, in_specs=in_specs, out_specs=out_specs, check_vma=False)
```

```python
import math

import jax
import jax.numpy as jnp
from jax import lax
from jax.experimental import pallas as pl
from jax.experimental.pallas import tpu as pltpu
from jax.sharding import PartitionSpec as P

BULK_TERM = -50.0
SHEAR_TERM = 1500.0
TIME_STEP = 0.1
STRETCH_CRITICAL = 0.04
STRETCH_WIDTH = 0.01
DIRECTION_EPS = 1e-06

REACH = 3
HALF = 0.5 / STRETCH_WIDTH
PEN = 0.5 * STRETCH_CRITICAL / STRETCH_WIDTH
LOST = 1024.0
F32 = jnp.float32
VMEM_LIMIT = 20 * 1024 * 1024


def half_bonds():
    listed = []
    for step_x in range(0, 4):
        for step_y in range(-3, 4):
            for step_z in range(-3, 4):
                forward_half = step_x > 0 or (
                    step_x == 0 and (step_y > 0 or (step_y == 0 and step_z > 0))
                )
                if forward_half and step_x * step_x + step_y * step_y + step_z * step_z <= 9:
                    listed.append((step_x, step_y, step_z))
    return listed


def flag_place(number):
    if number < 16:
        return (0, number)
    return (1 + (number - 16) // 15, (number - 16) % 15)


def bond_classes():
    classes = {}
    for number, (a, b, c) in enumerate(half_bonds()):
        word, bit = flag_place(number)
        group = classes.setdefault(a * a + b * b + c * c, [])
        group.append((a, b, c, word, bit, False))
        group.append((-a, -b, -c, word, bit, True))
    place = 0
    for squared in sorted(classes):
        classes[squared] = [bond + (place + k,) for k, bond in enumerate(classes[squared])]
        place += len(classes[squared])
    return {squared: classes[squared] for squared in sorted(classes)}, place


CLASSES, BONDS = bond_classes()
DIRECTED = [bond for bonds in CLASSES.values() for bond in bonds]


def layers_read(c, word=None):
    reach = [
        a for a, b, step, held, bit, backward, place in DIRECTED
        if step == c and (word is None or (backward and held == word))
    ]
    if c == 0:
        reach.append(0)
    return slice(3 + min(reach), 6 + max(reach)) if reach else None


SIDE = (-3, -2, -1, 3, 4, 5)
PAIRS = [(bond, x) for bond in DIRECTED for x in range(3)]
INNER = {(bond[-1], x): None for bond, x in PAIRS if 0 <= x + bond[0] < 3}
INNER = {key: n for n, key in enumerate(INNER)}
OUTER = {(bond[-1], x): None for bond, x in PAIRS if not 0 <= x + bond[0] < 3}
OUTER = {key: n for n, key in enumerate(OUTER)}
ROWS_Y = 6
BEYOND = (0, 5, 5, 3)
BEYOND_RATIO = (0, 2, 2, 0)


def pairwise(values, axis, odd):
    pairs = []
    for i in range(1 if odd else 0, lax.axis_size(axis) - 1, 2):
        pairs += [(i, i + 1), (i + 1, i)]
    return lax.ppermute(values, axis, pairs)


def both(odd_values, even_values, axis):
    return pairwise(odd_values, axis, True), pairwise(even_values, axis, False)


def call(kernel, outs, *operands, scratch=(), hbm=()):
    vmem = pl.BlockSpec(memory_space=pltpu.VMEM)
    spaces = [pltpu.HBM if n in hbm else pltpu.VMEM for n in range(len(operands))]
    held = [pltpu.with_memory_space_constraint(value, space) for value, space in zip(operands, spaces)]
    return pl.pallas_call(
        kernel,
        out_shape=outs,
        in_specs=[pl.BlockSpec(memory_space=space) for space in spaces],
        out_specs=jax.tree.map(lambda _: vmem, outs),
        scratch_shapes=list(scratch),
        compiler_params=pltpu.CompilerParams(vmem_limit_bytes=VMEM_LIMIT),
    )(*held)


def is_even(axis):
    return lax.axis_index(axis) % 2 == 0


def needed_rows(distance):
    return (6, 5, 5, 3)[distance]


def outer_rows(distance):
    return (3, 2, 2, 0)[distance]


def word_reach():
    reach = [0, 0, 0, 0]
    for number, (a, b, c) in enumerate(half_bonds()):
        word = flag_place(number)[0]
        reach[word] = max(reach[word], a)
    return reach


MOVING = [(f, x) for f in range(3) for x in range(3)]
SENT = MOVING + [(3, x) for x in range(3)]
SENT += [(4 + w, x) for w in range(4) for x in range(3 - word_reach()[w], 3)]
KEPT = [(4 + w, x) for w in range(4) for x in range(3) if (4 + w, x) not in SENT]


def strips(fields):
    placed, start = {}, 0
    for f in fields:
        for x in range(-3, 6):
            if f >= 4 and (x >= 3 or (x < 0 and (f, x + 3) not in SENT)):
                continue
            rows = needed_rows(max(0, -x, x - 2))
            placed[f, x] = (start, rows)
            start += rows
    return placed, start


ALL_STRIPS, ALL_ROWS = strips(range(8))
MOVING_STRIPS, MOVING_ROWS = strips(range(3))


def shifted(values, c):
    if c == 0:
        return values
    return pltpu.roll(values, (-c) % values.shape[-1], values.ndim - 1)


def pack_kernel(u_ref, bone_ref, broken_ref, sent_ref, kept_ref, bone_in, broken_in, sems):
    copies = [
        pltpu.make_async_copy(bone_ref, bone_in, sems.at[0]),
        pltpu.make_async_copy(broken_ref, broken_in, sems.at[1]),
    ]
    copies += [
        pltpu.make_async_copy(u_ref.at[f], sent_ref.at[3 * f : 3 * f + 3], sems.at[2 + f]) for f in range(3)
    ]
    for copy in copies:
        copy.start()
    copies[0].wait()
    sent_ref[9:12] = bone_in[...].astype(F32)
    copies[1].wait()
    for target, listed in ((sent_ref, SENT), (kept_ref, KEPT)):
        for n, (f, x) in enumerate(listed):
            if f >= 4:
                target[n] = broken_in[f - 4, x].astype(F32)
    for copy in copies[2:]:
        copy.wait()


def cut_strips(tile_of, placed, odd_ref, even_ref):
    even = is_even("gy")
    for (f, x), (start, rows) in placed.items():
        tile = tile_of(f, x)
        first, last = tile[0:rows], tile[tile.shape[0] - rows :]
        odd_ref[start : start + rows] = jnp.where(even, first, last)
        even_ref[start : start + rows] = jnp.where(even, last, first)


def widen_kernel(sent_ref, kept_ref, odd_ref, even_ref, side_ref, to_odd_ref, to_even_ref):
    even = is_even("gx")
    side_ref[0] = jnp.where(even, odd_ref[...], even_ref[...])
    side_ref[1] = jnp.where(even, even_ref[...], odd_ref[...])
    cut_strips(tiles(side_ref, sent_ref, kept_ref), ALL_STRIPS, to_odd_ref, to_even_ref)


def tiles(side_ref, own_ref, kept_ref):
    def tile_of(f, x):
        if x < 0:
            return side_ref[0, SENT.index((f, x + 3))]
        if x >= 3:
            return side_ref[1, SENT.index((f, x - 3))]
        if (f, x) in KEPT:
            return kept_ref[KEPT.index((f, x))]
        return own_ref[SENT.index((f, x))]

    return tile_of


def lay(field_ref, f, tile_of, placed, odd_ref, even_ref):
    even = is_even("gy")
    rows = field_ref.shape[1] // 3
    for x in range(-3, 6):
        if (f, x) in placed:
            field_ref[x + 3, 0:rows] = jnp.zeros((rows, field_ref.shape[2]), F32)
            field_ref[x + 3, 2 * rows : 3 * rows] = jnp.zeros((rows, field_ref.shape[2]), F32)
            start, count = placed[f, x]
            from_odd, from_even = odd_ref[start : start + count], even_ref[start : start + count]
            field_ref[x + 3, rows - count : rows] = jnp.where(even, from_odd, from_even)
            field_ref[x + 3, rows : 2 * rows] = tile_of(f, x)
            field_ref[x + 3, 2 * rows : 2 * rows + count] = jnp.where(even, from_even, from_odd)
    return field_ref[...]


def fill_moving(tile_of, placed, odd_ref, even_ref, field_ref, rolled_ref, own_ref, cells, region):
    first, last = region
    for f in range(3):
        field = lay(field_ref.at[f], f, tile_of, placed, odd_ref, even_ref)
        for c in range(-REACH, REACH + 1):
            part = layers_read(c)
            rolled_ref[c + REACH, f, part] = shifted(field[part], c)
    for f in range(3):
        here = rolled_ref[REACH, f, cells : 2 * cells, first:last]
        for step in range(-REACH, REACH + 1):
            own_ref[f, step + REACH] = here - float(step)


def bond_pass(rolled_ref, own_ref, pen_of, square_ref, along_ref, across_ref, out_ref, region, kinds):
    first, last = region
    shape = (last - first, own_ref.shape[-1])

    def layer(x, carry):
        totals = jnp.zeros(shape, F32)
        second = jnp.zeros(shape, F32)
        for squared, bonds in CLASSES.items():
            natural = math.sqrt(squared)
            moved = jnp.zeros(shape, F32)
            other = jnp.zeros(shape, F32)
            for a, b, c, word, bit, backward, place in bonds:
                rel = [
                    rolled_ref[c + REACH, f, x + 3 + a, first + b : last + b] - own_ref[f, step + REACH, x]
                    for f, step in enumerate((a, b, c))
                ]
                square = rel[0] * rel[0] + rel[1] * rel[1] + rel[2] * rel[2]
                length = square * lax.rsqrt(jnp.maximum(square, 1e-30))
                scaled = (length - natural) * (HALF / natural)
                pen = pen_of(a, b, c, word, bit, backward, place, x)
                weight = 1.0 + jnp.tanh(pen - scaled)
                pulled = weight * scaled
                square_ref[place, x] = square
                along_ref[place, x] = weight
                across_ref[place, x] = pulled
                moved = moved + pulled
                other = other + (pen if kinds == "volume" else weight)
            totals = totals + moved * (0.5 * natural / HALF)
            if kinds == "volume":
                lost = (PEN * len(bonds) - other) * (1.0 / LOST)
                second = second + (len(bonds) - lost) * natural
            else:
                second = second + other * (0.5 * natural)
        out_ref[0, x] = totals
        out_ref[1, x] = second
        return carry

    lax.fori_loop(0, 3, layer, 0)
    return out_ref[0], out_ref[1]


def cut_ratio(ratio_ref, to_odd_ref, to_even_ref, rows):
    even = is_even("gx")
    half = rows // 2
    start = 0
    for f in range(ratio_ref.shape[0]):
        for distance in range(1, 4):
            count = rows + 2 * outer_rows(distance)
            part = slice(half - outer_rows(distance), half + rows + outer_rows(distance))
            upper = ratio_ref[f, 3 - distance, part]
            lower = ratio_ref[f, distance - 1, part]
            to_odd_ref[start : start + count] = jnp.where(even, lower, upper)
            to_even_ref[start : start + count] = jnp.where(even, upper, lower)
            start += count


def ratio_rows(rows):
    return sum(rows + 2 * outer_rows(distance) for distance in range(1, 4))


def first_kernel(side_ref, sent_ref, kept_ref, odd_ref, even_ref, v_hbm, rolled_ref, pen_ref, square_ref, along_ref, across_ref, ratio_ref, to_odd_ref, to_even_ref, volume_ref, v_ref, mine_ref, field_ref, nb_ref, word_ref, sums_ref, sem):
    copy = pltpu.make_async_copy(v_hbm, v_ref, sem)
    copy.start()
    rows = sent_ref.shape[-2]
    depth = sent_ref.shape[-1]
    cells = pen_ref.shape[1]
    half = rows // 2
    region = (half, half + 2 * rows)
    tile_of = tiles(side_ref, sent_ref, kept_ref)
    fill_moving(tile_of, ALL_STRIPS, odd_ref, even_ref, field_ref, rolled_ref, mine_ref, cells, region)
    bone = lay(field_ref.at[0], 3, tile_of, ALL_STRIPS, odd_ref, even_ref)
    void = jnp.where(bone == 0.0, -1, 0)
    for c in range(-REACH, REACH + 1):
        part = layers_read(c)
        turned = shifted(void[part], c)
        if c != 0:
            lane = lax.broadcasted_iota(jnp.int32, turned.shape, 2) + c
            turned = jnp.where((lane >= 0) & (lane < depth), turned, -1)
        nb_ref[c + REACH, part] = turned
    for w in range(4):
        words = lay(field_ref.at[1 + w % 2], 4 + w, tile_of, ALL_STRIPS, odd_ref, even_ref)
        words = words[0 : 2 * cells].astype(jnp.int32)
        for c in range(-REACH, REACH + 1):
            part = layers_read(c, w)
            if part is not None:
                word_ref[c + REACH, w, part] = shifted(words[part], c) | nb_ref[c + REACH, part]

    first, last = region

    def pen_of(a, b, c, word, bit, backward, place, x):
        if backward:
            words = word_ref[c + REACH, word, x + 3 + a, first + b : last + b]
            hit = words & (1 << bit)
        else:
            words = word_ref[REACH, word, x + 3, first:last]
            far = nb_ref[c + REACH, x + 3 + a, first + b : last + b]
            hit = (words & (1 << bit)) | far
        pen = jnp.where(hit == 0, PEN, PEN - LOST)
        pen_ref[place, x] = pen
        return pen

    totals, volume = bond_pass(rolled_ref, mine_ref, pen_of, square_ref, along_ref, across_ref, sums_ref, region, "volume")
    solid = jnp.where(nb_ref[REACH, cells : 2 * cells, first:last] == 0, 1.0, 0.0)
    volume = jnp.maximum(volume * solid, 1.0)
    inverse = 1.0 / volume
    dilatation = 3.0 * (totals * solid) / volume
    ratio_ref[0] = dilatation * inverse * (0.5 * BULK_TERM)
    ratio_ref[1] = inverse * (0.5 * SHEAR_TERM / HALF)
    cut_ratio(ratio_ref, to_odd_ref, to_even_ref, rows)
    volume_ref[0] = volume
    volume_ref[1] = solid
    copy.wait()


def forces(total, inner, rolled_ref, square_ref, along_ref, across_ref, scaled_ref, inverse_ref, rows):
    half = rows // 2
    mine = slice(half, half + rows)
    for x in range(3):
        scaled = scaled_ref[REACH, x + 3, mine]
        inverse = inverse_ref[REACH, x + 3, mine]
        here = [rolled_ref[REACH, f, x + 3, rows : 2 * rows] for f in range(3)]
        for bonds in CLASSES.values():
            for a, b, c, word, bit, backward, place in bonds:
                if (0 <= x + a < 3) != inner:
                    continue
                far = (c + REACH, x + 3 + a, slice(half + b, half + rows + b))
                magnitude = along_ref[place, x, mine] * (scaled + scaled_ref[far])
                magnitude = magnitude + across_ref[place, x, mine] * (inverse + inverse_ref[far])
                magnitude = magnitude * lax.rsqrt(square_ref[place, x, mine] + DIRECTION_EPS)
                for f, step in enumerate((a, b, c)):
                    rel = rolled_ref[c + REACH, f, x + 3 + a, rows + b : 2 * rows + b] - here[f]
                    if step:
                        rel = rel + float(step)
                    total[f][x] = total[f][x] + magnitude * rel
    return total


def fill_inner(target_ref, own):
    for c in range(-REACH, REACH + 1):
        target_ref[c + REACH, 3:6] = shifted(own, c)


def fill_outer(target_ref, field_ref, f, odd_ref, even_ref, rows):
    even = is_even("gx")
    half = rows // 2
    field_ref[...] = jnp.zeros(field_ref.shape, F32)
    start = f * ratio_rows(rows)
    for distance in range(1, 4):
        count = rows + 2 * outer_rows(distance)
        part = slice(half - outer_rows(distance), half + rows + outer_rows(distance))
        from_odd, from_even = odd_ref[start : start + count], even_ref[start : start + count]
        field_ref[3 - distance, part] = jnp.where(even, from_odd, from_even)
        field_ref[2 + distance, part] = jnp.where(even, from_even, from_odd)
        start += count
    field = field_ref[...]
    for c in range(-REACH, REACH + 1):
        turned = shifted(field, c)
        target_ref[c + REACH, 0:3] = turned[0:3]
        target_ref[c + REACH, 6:9] = turned[3:6]


def start_total(rows, depth):
    return [[jnp.zeros((rows, depth), F32) for _ in range(3)] for _ in range(3)]


def inner_kernel(rolled_ref, square_ref, along_ref, across_ref, ratio_ref, held_ref, part_ref, scaled_ref, inverse_ref):
    rows, depth = part_ref.shape[2:]
    fill_inner(scaled_ref, ratio_ref[0])
    if held_ref is None:
        held_ref = inverse_ref
        fill_inner(inverse_ref, ratio_ref[1])
    total = forces(start_total(rows, depth), True, rolled_ref, square_ref, along_ref, across_ref, scaled_ref, held_ref, rows)
    for f in range(3):
        for x in range(3):
            part_ref[f, x] = total[f][x]


def first_inner_kernel(rolled_ref, square_ref, along_ref, across_ref, ratio_ref, part_ref, scaled_ref, inverse_ref):
    inner_kernel(rolled_ref, square_ref, along_ref, across_ref, ratio_ref, None, part_ref, scaled_ref, inverse_ref)


def outer_forces(rolled_ref, square_ref, along_ref, across_ref, scaled_ref, inverse_ref, part_ref, rows):
    total = [[part_ref[f, x] for x in range(3)] for f in range(3)]
    return forces(total, False, rolled_ref, square_ref, along_ref, across_ref, scaled_ref, inverse_ref, rows)


def move_kernel(rolled_ref, square_ref, along_ref, across_ref, ratio_ref, part_ref, odd_ref, even_ref, volume_ref, sent_ref, v_ref, u_out, v_out, inverse_ref, to_odd_ref, to_even_ref, scaled_ref, field_ref):
    rows = v_ref.shape[2]
    half = rows // 2
    for f, target in ((0, scaled_ref), (1, inverse_ref)):
        fill_outer(target, field_ref.at[f], f, odd_ref, even_ref, rows)
        fill_inner(target, ratio_ref[f])
    total = outer_forces(rolled_ref, square_ref, along_ref, across_ref, scaled_ref, inverse_ref, part_ref, rows)
    for f in range(3):
        for x in range(3):
            speed = v_ref[f, x] + TIME_STEP * (total[f][x] * volume_ref[1, x, half : half + rows])
            v_out[f, x] = speed
            u_out[f, x] = sent_ref[3 * f + x] + TIME_STEP * speed
    cut_y(lambda f, x: u_out[f, x], 3, to_odd_ref, to_even_ref)


def strips_x(fields, rows, beyond):
    placed, start = {}, 0
    for f in range(fields):
        for distance in range(1, 4):
            if f >= 4 and word_reach()[f - 4] < distance:
                continue
            count = rows + 2 * beyond[distance]
            placed[f, distance] = (start, count, beyond[distance])
            start += count
    return placed, start


def cut_y(value_of, fields, odd_ref, even_ref):
    even = is_even("gy")
    for f in range(fields):
        for x in range(3):
            tile = value_of(f, x)
            first, last = tile[0:ROWS_Y], tile[tile.shape[0] - ROWS_Y :]
            part = slice((3 * f + x) * ROWS_Y, (3 * f + x + 1) * ROWS_Y)
            odd_ref[part] = jnp.where(even, first, last)
            even_ref[part] = jnp.where(even, last, first)


def cut_x(source_ref, fields, rows, beyond, base, odd_ref, even_ref):
    even = is_even("gx")
    for (f, distance), (start, count, more) in strips_x(fields, rows, beyond)[0].items():
        part = slice(base - more, base + rows + more)
        upper, lower = source_ref[f, 3 - distance, part], source_ref[f, distance - 1, part]
        odd_ref[start : start + count] = jnp.where(even, lower, upper)
        even_ref[start : start + count] = jnp.where(even, upper, lower)


def lay_side(field_ref, f, fields, rows, beyond, base, odd_ref, even_ref):
    even = is_even("gx")
    field_ref[...] = jnp.zeros(field_ref.shape, F32)
    placed = strips_x(fields, rows, beyond)[0]
    for distance in range(1, 4):
        if (f, distance) in placed:
            start, count, more = placed[f, distance]
            part = slice(base - more, base + rows + more)
            from_odd, from_even = odd_ref[start : start + count], even_ref[start : start + count]
            field_ref[3 - distance, part] = jnp.where(even, from_odd, from_even)
            field_ref[2 + distance, part] = jnp.where(even, from_even, from_odd)
    return field_ref[...]


def outer_part(c):
    return {0: slice(0, 6), 3: None}.get(abs(c), slice(1, 5))


def widen_moved_kernel(own_ref, odd_ref, even_ref, tall_ref, to_odd_ref, to_even_ref):
    even = is_even("gy")
    fields, rows = own_ref.shape[0], own_ref.shape[2]
    blank = jnp.zeros((rows - ROWS_Y, own_ref.shape[3]), F32)
    for f in range(fields):
        for x in range(3):
            part = slice((3 * f + x) * ROWS_Y, (3 * f + x + 1) * ROWS_Y)
            from_odd, from_even = odd_ref[part], even_ref[part]
            tall_ref[f, x, 0 : rows - ROWS_Y] = blank
            tall_ref[f, x, rows - ROWS_Y : rows] = jnp.where(even, from_odd, from_even)
            tall_ref[f, x, rows : 2 * rows] = own_ref[f, x]
            tall_ref[f, x, 2 * rows : 2 * rows + ROWS_Y] = jnp.where(even, from_even, from_odd)
            tall_ref[f, x, 2 * rows + ROWS_Y :] = blank
    cut_x(tall_ref, fields, rows, BEYOND, rows, to_odd_ref, to_even_ref)


def region_of(rows):
    return rows // 2, rows // 2 + 2 * rows


def split_pass(places, far_of, own_ref, pen_of, square_ref, along_ref, across_ref, sums_ref, begun_ref, kinds):
    shape = own_ref.shape[3:]
    for x in range(3):
        totals = jnp.zeros(shape, F32) if begun_ref is None else begun_ref[0, x]
        second = jnp.zeros(shape, F32) if begun_ref is None else begun_ref[1, x]
        for squared, bonds in CLASSES.items():
            natural = math.sqrt(squared)
            held = [bond for bond in bonds if (bond[-1], x) in places]
            if not held:
                continue
            moved = jnp.zeros(shape, F32)
            other = jnp.zeros(shape, F32)
            for bond in held:
                a, b, c = bond[:3]
                n = places[bond[-1], x]
                rel = [far_of(c, f, x + a, b) - own_ref[f, step + REACH, x] for f, step in enumerate((a, b, c))]
                square = rel[0] * rel[0] + rel[1] * rel[1] + rel[2] * rel[2]
                length = square * lax.rsqrt(jnp.maximum(square, 1e-30))
                scaled = (length - natural) * (HALF / natural)
                pen = pen_of(bond, n, x)
                weight = 1.0 + jnp.tanh(pen - scaled)
                pulled = weight * scaled
                square_ref[n] = square
                along_ref[n] = weight
                across_ref[n] = pulled
                moved = moved + pulled
                other = other + (pen if kinds == "volume" else weight)
            totals = totals + moved * (0.5 * natural / HALF)
            if kinds == "volume":
                lost = (PEN * len(held) - other) * (1.0 / LOST)
                second = second + (len(held) - lost) * natural
            else:
                second = second + other * (0.5 * natural)
        sums_ref[0, x] = totals
        sums_ref[1, x] = second


def fill_inner_moving(tall_ref, rolled_ref, mine_ref):
    first, last = region_of(tall_ref.shape[2] // 3)
    for f in range(3):
        field = tall_ref[f]
        for c in range(-REACH, REACH + 1):
            rolled_ref[c + REACH, f] = shifted(field, c)
        here = tall_ref[f, :, first:last]
        for step in range(-REACH, REACH + 1):
            mine_ref[f, step + REACH] = here - float(step)


def fill_outer_moving(odd_ref, even_ref, fields, field_ref, rolled_ref):
    rows = field_ref.shape[2] // 3
    for f in range(3):
        field = lay_side(field_ref.at[f], f, fields, rows, BEYOND, rows, odd_ref, even_ref)
        for c in range(-REACH, REACH + 1):
            part = outer_part(c)
            if part is not None:
                rolled_ref[c + REACH, f, part] = shifted(field[part], c)


def inner_far(rolled_ref):
    first, last = region_of(rolled_ref.shape[3] // 3)
    return lambda c, f, layer, b: rolled_ref[c + REACH, f, layer, first + b : last + b]


def outer_far(rolled_ref):
    first, last = region_of(rolled_ref.shape[3] // 3)
    return lambda c, f, layer, b: rolled_ref[c + REACH, f, SIDE.index(layer), first + b : last + b]


def later_inside_kernel(tall_ref, pen_ref, rolled_ref, mine_ref, square_ref, along_ref, across_ref, sums_ref):
    fill_inner_moving(tall_ref, rolled_ref, mine_ref)
    split_pass(INNER, inner_far(rolled_ref), mine_ref, lambda bond, n, x: pen_ref[bond[-1], x], square_ref, along_ref, across_ref, sums_ref, None, "weight")


def later_kernel(odd_ref, even_ref, mine_ref, pen_ref, begun_ref, volume_ref, rolled_ref, square_ref, along_ref, across_ref, ratio_ref, to_odd_ref, to_even_ref, damage_ref, field_ref, sums_ref):
    rows = field_ref.shape[2] // 3
    half = rows // 2
    fill_outer_moving(odd_ref, even_ref, 3, field_ref, rolled_ref)
    split_pass(OUTER, outer_far(rolled_ref), mine_ref, lambda bond, n, x: pen_ref[bond[-1], x], square_ref, along_ref, across_ref, sums_ref, begun_ref, "weight")
    volume = volume_ref[0]
    solid = volume_ref[1]
    inverse = 1.0 / volume
    dilatation = 3.0 * (sums_ref[0] * solid) / volume
    ratio_ref[0] = dilatation * inverse * (0.5 * BULK_TERM)
    cut_x(ratio_ref, 1, rows, BEYOND_RATIO, half, to_odd_ref, to_even_ref)
    damage = 1.0 - (sums_ref[1] * solid) / volume
    damage_ref[...] = damage[:, half : half + rows]


def split_forces(total, places, index, rolled_ref, here_ref, square_ref, along_ref, across_ref, ratio_ref, held_ref, scaled_ref, inverse_ref):
    rows = here_ref.shape[3] // 3
    half = rows // 2
    mine = slice(half, half + rows)
    for x in range(3):
        scaled = ratio_ref[0, x, mine]
        inverse = held_ref[1, x, mine]
        here = [here_ref[REACH, f, x, rows : 2 * rows] for f in range(3)]
        for a, b, c, word, bit, backward, place in DIRECTED:
            if (place, x) not in places:
                continue
            n = places[place, x]
            far = (c + REACH, index(x + a), slice(half + b, half + rows + b))
            magnitude = along_ref[n, mine] * (scaled + scaled_ref[far])
            magnitude = magnitude + across_ref[n, mine] * (inverse + inverse_ref[c + REACH, x + 3 + a, far[2]])
            magnitude = magnitude * lax.rsqrt(square_ref[n, mine] + DIRECTION_EPS)
            for f, step in enumerate((a, b, c)):
                rel = rolled_ref[c + REACH, f, index(x + a), rows + b : 2 * rows + b] - here[f]
                if step:
                    rel = rel + float(step)
                total[f][x] = total[f][x] + magnitude * rel
    return total


def fill_own(target_ref, own):
    for c in range(-REACH, REACH + 1):
        target_ref[c + REACH] = shifted(own, c)


def fill_side(target_ref, field_ref, f, fields, odd_ref, even_ref, rows):
    field = lay_side(field_ref, f, fields, rows, BEYOND_RATIO, rows // 2, odd_ref, even_ref)
    for c in range(-REACH, REACH + 1):
        part = outer_part(c)
        if part is not None:
            target_ref[c + REACH, part] = shifted(field[part], c)


def inside_forces(rolled_ref, square_ref, along_ref, across_ref, ratio_ref, held_ref, scaled_ref, inverse_ref, part_ref):
    rows, depth = part_ref.shape[2:]
    total = [[jnp.zeros((rows, depth), F32) for _ in range(3)] for _ in range(3)]
    total = split_forces(total, INNER, lambda layer: layer, rolled_ref, rolled_ref, square_ref, along_ref, across_ref, ratio_ref, held_ref, scaled_ref, inverse_ref)
    for f in range(3):
        for x in range(3):
            part_ref[f, x] = total[f][x]


def last_inside_kernel(rolled_ref, square_ref, along_ref, across_ref, ratio_ref, held_ref, inverse_ref, part_ref, scaled_ref):
    fill_own(scaled_ref, ratio_ref[0])
    inside_forces(rolled_ref, square_ref, along_ref, across_ref, ratio_ref, held_ref, scaled_ref, inverse_ref, part_ref)


def last_kernel(odd_ref, even_ref, rolled_ref, inside_ref, square_ref, along_ref, across_ref, ratio_ref, held_ref, part_ref, volume_ref, v_ref, inverse_ref, damage_ref, v_out, damage_out, scaled_ref, field_ref):
    rows = v_ref.shape[2]
    half = rows // 2
    damage_out[...] = damage_ref[...]
    fill_side(scaled_ref, field_ref, 0, 1, odd_ref, even_ref, rows)
    total = [[part_ref[f, x] for x in range(3)] for f in range(3)]
    total = split_forces(total, OUTER, SIDE.index, rolled_ref, inside_ref, square_ref, along_ref, across_ref, ratio_ref, held_ref, scaled_ref, inverse_ref)
    for f in range(3):
        for x in range(3):
            v_out[f, x] = v_ref[f, x] + TIME_STEP * (total[f][x] * volume_ref[1, x, half : half + rows])


def body(displacement, velocity, bone, broken):
    cells, rows, depth = bone.shape
    if cells != REACH or rows != 8:
        raise ValueError("block size")
    layers, tall, region = 3 * cells, 3 * rows, 2 * rows
    turns = 2 * REACH + 1

    def vmem(*shape, dtype=F32):
        return pltpu.VMEM(shape, dtype)

    hbm = jax.ShapeDtypeStruct
    sent, kept = call(
        pack_kernel,
        (vmem(len(SENT), rows, depth), vmem(len(KEPT), rows, depth)),
        displacement,
        bone,
        broken,
        scratch=(
            vmem(cells, rows, depth, dtype=jnp.int32),
            vmem(4, cells, rows, depth, dtype=jnp.int32),
            pltpu.SemaphoreType.DMA((5,)),
        ),
        hbm=(0, 1, 2),
    )
    side, to_odd, to_even = call(
        widen_kernel,
        (vmem(2, len(SENT), rows, depth), vmem(ALL_ROWS, depth), vmem(ALL_ROWS, depth)),
        sent,
        kept,
        *both(sent, sent, "gx"),
    )
    bonds = (BONDS, cells, region, depth)
    crossing = ratio_rows(rows)
    rolled, pen, square, along, across, ratio, to_odd, to_even, volume, speed = call(
        first_kernel,
        (
            vmem(turns, 3, layers, tall, depth),
            vmem(*bonds),
            vmem(*bonds),
            vmem(*bonds),
            vmem(*bonds),
            vmem(2, cells, region, depth),
            vmem(2 * crossing, depth),
            vmem(2 * crossing, depth),
            vmem(2, cells, region, depth),
            vmem(3, cells, rows, depth),
        ),
        side,
        sent,
        kept,
        *both(to_odd, to_even, "gy"),
        velocity,
        scratch=(
            vmem(3, turns, cells, region, depth),
            vmem(3, layers, tall, depth),
            vmem(turns, layers, tall, depth, dtype=jnp.int32),
            vmem(turns, 4, 2 * cells, tall, depth, dtype=jnp.int32),
            vmem(2, cells, region, depth),
            pltpu.SemaphoreType.DMA(()),
        ),
        hbm=(5,),
    )
    arrived = both(to_odd, to_even, "gx")
    wide_ratio = vmem(turns, layers, region, depth)
    part = call(
        first_inner_kernel,
        vmem(3, cells, rows, depth),
        rolled,
        square,
        along,
        across,
        ratio,
        scratch=(wide_ratio, wide_ratio),
    )
    moved, speed, inverse, *to = call(
        move_kernel,
        (vmem(3, cells, rows, depth), vmem(3, cells, rows, depth), wide_ratio) + (vmem(3 * 3 * ROWS_Y, depth),) * 2,
        rolled,
        square,
        along,
        across,
        ratio,
        part,
        *arrived,
        volume,
        sent,
        speed,
        scratch=(wide_ratio, vmem(2, 6, region, depth)),
    )
    sides = len(SIDE)
    block = vmem(3, cells, rows, depth)
    in_bonds, out_bonds = vmem(len(INNER), region, depth), vmem(len(OUTER), region, depth)
    in_rolled, out_rolled = vmem(turns, 3, cells, tall, depth), vmem(turns, 3, sides, tall, depth)
    in_ratio, out_ratio = vmem(turns, cells, region, depth), vmem(turns, sides, region, depth)
    mine_shape = vmem(3, turns, cells, region, depth)
    two = vmem(2, cells, region, depth)

    def strips(fields, beyond):
        return (vmem(strips_x(fields, rows, beyond)[1], depth),) * 2

    tall_moved, *to = call(
        widen_moved_kernel, (vmem(3, cells, tall, depth),) + strips(3, BEYOND), moved, *both(*to, "gy")
    )
    arrived = both(*to, "gx")
    inside, mine, *in_held, begun = call(
        later_inside_kernel, (in_rolled, mine_shape) + (in_bonds,) * 3 + (two,), tall_moved, pen
    )
    held_ratio = ratio
    rolled, *out_held, ratio, to_odd, to_even, damage = call(
        later_kernel,
        (out_rolled,) + (out_bonds,) * 3 + (vmem(1, cells, region, depth),) + strips(1, BEYOND_RATIO) + (vmem(cells, rows, depth),),
        *arrived,
        mine,
        pen,
        begun,
        volume,
        scratch=(vmem(3, sides, tall, depth), two),
    )
    arrived = both(to_odd, to_even, "gx")
    part = call(last_inside_kernel, block, inside, *in_held, ratio, held_ratio, inverse, scratch=(in_ratio,))
    return call(
        last_kernel,
        (hbm((3, cells, rows, depth), F32), hbm((cells, rows, depth), F32)),
        *arrived,
        rolled,
        inside,
        *out_held,
        ratio,
        held_ratio,
        part,
        volume,
        speed,
        inverse,
        damage,
        scratch=(out_ratio, vmem(sides, region, depth)),
    )


def solution(mesh):
    in_specs = (
        P(None, "gx", "gy", None),
        P(None, "gx", "gy", None),
        P("gx", "gy", None),
        P(None, "gx", "gy", None),
    )
    out_specs = (P(None, "gx", "gy", None), P("gx", "gy", None))
    return jax.shard_map(body, mesh=mesh, in_specs=in_specs, out_specs=out_specs, check_vma=False)
```

```python
import math

import jax
import jax.numpy as jnp
from jax import lax
from jax.experimental import pallas as pl
from jax.experimental.pallas import tpu as pltpu
from jax.sharding import PartitionSpec as P

BULK_TERM = -50.0
SHEAR_TERM = 1500.0
TIME_STEP = 0.1
STRETCH_CRITICAL = 0.04
STRETCH_WIDTH = 0.01
DIRECTION_EPS = 1e-06

REACH = 3
HALF = 0.5 / STRETCH_WIDTH
PEN = 0.5 * STRETCH_CRITICAL / STRETCH_WIDTH
LOST = 1024.0
F32 = jnp.float32
VMEM_LIMIT = 20 * 1024 * 1024


def half_bonds():
    listed = []
    for step_x in range(0, 4):
        for step_y in range(-3, 4):
            for step_z in range(-3, 4):
                forward_half = step_x > 0 or (
                    step_x == 0 and (step_y > 0 or (step_y == 0 and step_z > 0))
                )
                if forward_half and step_x * step_x + step_y * step_y + step_z * step_z <= 9:
                    listed.append((step_x, step_y, step_z))
    return listed


def flag_place(number):
    if number < 16:
        return (0, number)
    return (1 + (number - 16) // 15, (number - 16) % 15)


def bond_classes():
    classes = {}
    for number, (a, b, c) in enumerate(half_bonds()):
        word, bit = flag_place(number)
        group = classes.setdefault(a * a + b * b + c * c, [])
        group.append((a, b, c, word, bit, False))
        group.append((-a, -b, -c, word, bit, True))
    place = 0
    for squared in sorted(classes):
        classes[squared] = [bond + (place + k,) for k, bond in enumerate(classes[squared])]
        place += len(classes[squared])
    return {squared: classes[squared] for squared in sorted(classes)}, place


CLASSES, BONDS = bond_classes()
DIRECTED = [bond for bonds in CLASSES.values() for bond in bonds]


def layers_read(c, word=None):
    reach = [
        a for a, b, step, held, bit, backward, place in DIRECTED
        if step == c and (word is None or (backward and held == word))
    ]
    if c == 0:
        reach.append(0)
    return slice(3 + min(reach), 6 + max(reach)) if reach else None


SIDE = (-3, -2, -1, 3, 4, 5)
PAIRS = [(bond, x) for bond in DIRECTED for x in range(3)]
INNER = {(bond[-1], x): None for bond, x in PAIRS if 0 <= x + bond[0] < 3}
INNER = {key: n for n, key in enumerate(INNER)}
OUTER = {(bond[-1], x): None for bond, x in PAIRS if not 0 <= x + bond[0] < 3}
OUTER = {key: n for n, key in enumerate(OUTER)}
ROWS_Y = 6
BEYOND = (0, 5, 5, 3)
BEYOND_RATIO = (0, 2, 2, 0)


def pairwise(values, axis, odd):
    pairs = []
    for i in range(1 if odd else 0, lax.axis_size(axis) - 1, 2):
        pairs += [(i, i + 1), (i + 1, i)]
    return lax.ppermute(values, axis, pairs)


def both(odd_values, even_values, axis):
    return pairwise(odd_values, axis, True), pairwise(even_values, axis, False)


def call(kernel, outs, *operands, scratch=(), hbm=()):
    vmem = pl.BlockSpec(memory_space=pltpu.VMEM)
    spaces = [pltpu.HBM if n in hbm else pltpu.VMEM for n in range(len(operands))]
    held = [pltpu.with_memory_space_constraint(value, space) for value, space in zip(operands, spaces)]
    return pl.pallas_call(
        kernel,
        out_shape=outs,
        in_specs=[pl.BlockSpec(memory_space=space) for space in spaces],
        out_specs=jax.tree.map(lambda _: vmem, outs),
        scratch_shapes=list(scratch),
        compiler_params=pltpu.CompilerParams(vmem_limit_bytes=VMEM_LIMIT),
    )(*held)


def is_even(axis):
    return lax.axis_index(axis) % 2 == 0


def needed_rows(distance):
    return (6, 5, 5, 3)[distance]


def outer_rows(distance):
    return (3, 2, 2, 0)[distance]


def word_reach():
    reach = [0, 0, 0, 0]
    for number, (a, b, c) in enumerate(half_bonds()):
        word = flag_place(number)[0]
        reach[word] = max(reach[word], a)
    return reach


MOVING = [(f, x) for f in range(3) for x in range(3)]
SENT = MOVING + [(3, x) for x in range(3)]
SENT += [(4 + w, x) for w in range(4) for x in range(3 - word_reach()[w], 3)]
KEPT = [(4 + w, x) for w in range(4) for x in range(3) if (4 + w, x) not in SENT]


def strips(fields):
    placed, start = {}, 0
    for f in fields:
        for x in range(-3, 6):
            if f >= 4 and (x >= 3 or (x < 0 and (f, x + 3) not in SENT)):
                continue
            rows = needed_rows(max(0, -x, x - 2))
            placed[f, x] = (start, rows)
            start += rows
    return placed, start


ALL_STRIPS, ALL_ROWS = strips(range(8))
MOVING_STRIPS, MOVING_ROWS = strips(range(3))


def shifted(values, c):
    if c == 0:
        return values
    return pltpu.roll(values, (-c) % values.shape[-1], values.ndim - 1)


def pack_kernel(u_ref, bone_ref, broken_ref, sent_ref, kept_ref, bone_in, broken_in, sems):
    copies = [
        pltpu.make_async_copy(bone_ref, bone_in, sems.at[0]),
        pltpu.make_async_copy(broken_ref, broken_in, sems.at[1]),
    ]
    copies += [
        pltpu.make_async_copy(u_ref.at[f], sent_ref.at[3 * f : 3 * f + 3], sems.at[2 + f]) for f in range(3)
    ]
    for copy in copies:
        copy.start()
    copies[0].wait()
    sent_ref[9:12] = bone_in[...].astype(F32)
    copies[1].wait()
    for target, listed in ((sent_ref, SENT), (kept_ref, KEPT)):
        for n, (f, x) in enumerate(listed):
            if f >= 4:
                target[n] = broken_in[f - 4, x].astype(F32)
    for copy in copies[2:]:
        copy.wait()


def cut_strips(tile_of, placed, odd_ref, even_ref):
    even = is_even("gy")
    for (f, x), (start, rows) in placed.items():
        tile = tile_of(f, x)
        first, last = tile[0:rows], tile[tile.shape[0] - rows :]
        odd_ref[start : start + rows] = jnp.where(even, first, last)
        even_ref[start : start + rows] = jnp.where(even, last, first)


def widen_kernel(sent_ref, kept_ref, odd_ref, even_ref, side_ref, to_odd_ref, to_even_ref):
    even = is_even("gx")
    side_ref[0] = jnp.where(even, odd_ref[...], even_ref[...])
    side_ref[1] = jnp.where(even, even_ref[...], odd_ref[...])
    cut_strips(tiles(side_ref, sent_ref, kept_ref), ALL_STRIPS, to_odd_ref, to_even_ref)


def tiles(side_ref, own_ref, kept_ref):
    def tile_of(f, x):
        if x < 0:
            return side_ref[0, SENT.index((f, x + 3))]
        if x >= 3:
            return side_ref[1, SENT.index((f, x - 3))]
        if (f, x) in KEPT:
            return kept_ref[KEPT.index((f, x))]
        return own_ref[SENT.index((f, x))]

    return tile_of


def lay(field_ref, f, tile_of, placed, odd_ref, even_ref):
    even = is_even("gy")
    rows = field_ref.shape[1] // 3
    for x in range(-3, 6):
        if (f, x) in placed:
            field_ref[x + 3, 0:rows] = jnp.zeros((rows, field_ref.shape[2]), F32)
            field_ref[x + 3, 2 * rows : 3 * rows] = jnp.zeros((rows, field_ref.shape[2]), F32)
            start, count = placed[f, x]
            from_odd, from_even = odd_ref[start : start + count], even_ref[start : start + count]
            field_ref[x + 3, rows - count : rows] = jnp.where(even, from_odd, from_even)
            field_ref[x + 3, rows : 2 * rows] = tile_of(f, x)
            field_ref[x + 3, 2 * rows : 2 * rows + count] = jnp.where(even, from_even, from_odd)
    return field_ref[...]


def fill_moving(tile_of, placed, odd_ref, even_ref, field_ref, rolled_ref, own_ref, cells, region):
    first, last = region
    for f in range(3):
        field = lay(field_ref.at[f], f, tile_of, placed, odd_ref, even_ref)
        for c in range(-REACH, REACH + 1):
            part = layers_read(c)
            rolled_ref[c + REACH, f, part] = shifted(field[part], c)
    for f in range(3):
        here = rolled_ref[REACH, f, cells : 2 * cells, first:last]
        for step in range(-REACH, REACH + 1):
            own_ref[f, step + REACH] = here - float(step)


def bond_pass(rolled_ref, own_ref, pen_of, square_ref, along_ref, across_ref, out_ref, region, kinds):
    first, last = region
    shape = (last - first, own_ref.shape[-1])

    def layer(x, carry):
        totals = jnp.zeros(shape, F32)
        second = jnp.zeros(shape, F32)
        for squared, bonds in CLASSES.items():
            natural = math.sqrt(squared)
            moved = jnp.zeros(shape, F32)
            other = jnp.zeros(shape, F32)
            for a, b, c, word, bit, backward, place in bonds:
                rel = [
                    rolled_ref[c + REACH, f, x + 3 + a, first + b : last + b] - own_ref[f, step + REACH, x]
                    for f, step in enumerate((a, b, c))
                ]
                square = rel[0] * rel[0] + rel[1] * rel[1] + rel[2] * rel[2]
                length = square * lax.rsqrt(jnp.maximum(square, 1e-30))
                scaled = (length - natural) * (HALF / natural)
                pen = pen_of(a, b, c, word, bit, backward, place, x)
                weight = 1.0 + jnp.tanh(pen - scaled)
                pulled = weight * scaled
                square_ref[place, x] = square
                along_ref[place, x] = weight
                across_ref[place, x] = pulled
                moved = moved + pulled
                other = other + (pen if kinds == "volume" else weight)
            totals = totals + moved * (0.5 * natural / HALF)
            if kinds == "volume":
                lost = (PEN * len(bonds) - other) * (1.0 / LOST)
                second = second + (len(bonds) - lost) * natural
            else:
                second = second + other * (0.5 * natural)
        out_ref[0, x] = totals
        out_ref[1, x] = second
        return carry

    lax.fori_loop(0, 3, layer, 0)
    return out_ref[0], out_ref[1]


def cut_ratio(ratio_ref, to_odd_ref, to_even_ref, rows):
    even = is_even("gx")
    half = rows // 2
    start = 0
    for f in range(ratio_ref.shape[0]):
        for distance in range(1, 4):
            count = rows + 2 * outer_rows(distance)
            part = slice(half - outer_rows(distance), half + rows + outer_rows(distance))
            upper = ratio_ref[f, 3 - distance, part]
            lower = ratio_ref[f, distance - 1, part]
            to_odd_ref[start : start + count] = jnp.where(even, lower, upper)
            to_even_ref[start : start + count] = jnp.where(even, upper, lower)
            start += count


def ratio_rows(rows):
    return sum(rows + 2 * outer_rows(distance) for distance in range(1, 4))


def first_kernel(side_ref, sent_ref, kept_ref, odd_ref, even_ref, v_hbm, rolled_ref, pen_ref, square_ref, along_ref, across_ref, ratio_ref, to_odd_ref, to_even_ref, volume_ref, v_ref, mine_ref, field_ref, nb_ref, word_ref, sums_ref, sem):
    copy = pltpu.make_async_copy(v_hbm, v_ref, sem)
    copy.start()
    rows = sent_ref.shape[-2]
    depth = sent_ref.shape[-1]
    cells = pen_ref.shape[1]
    half = rows // 2
    region = (half, half + 2 * rows)
    tile_of = tiles(side_ref, sent_ref, kept_ref)
    fill_moving(tile_of, ALL_STRIPS, odd_ref, even_ref, field_ref, rolled_ref, mine_ref, cells, region)
    bone = lay(field_ref.at[0], 3, tile_of, ALL_STRIPS, odd_ref, even_ref)
    void = jnp.where(bone == 0.0, -1, 0)
    for c in range(-REACH, REACH + 1):
        part = layers_read(c)
        turned = shifted(void[part], c)
        if c != 0:
            lane = lax.broadcasted_iota(jnp.int32, turned.shape, 2) + c
            turned = jnp.where((lane >= 0) & (lane < depth), turned, -1)
        nb_ref[c + REACH, part] = turned
    for w in range(4):
        words = lay(field_ref.at[1 + w % 2], 4 + w, tile_of, ALL_STRIPS, odd_ref, even_ref)
        words = words[0 : 2 * cells].astype(jnp.int32)
        for c in range(-REACH, REACH + 1):
            part = layers_read(c, w)
            if part is not None:
                word_ref[c + REACH, w, part] = shifted(words[part], c) | nb_ref[c + REACH, part]

    first, last = region

    def pen_of(a, b, c, word, bit, backward, place, x):
        if backward:
            words = word_ref[c + REACH, word, x + 3 + a, first + b : last + b]
            hit = words & (1 << bit)
        else:
            words = word_ref[REACH, word, x + 3, first:last]
            far = nb_ref[c + REACH, x + 3 + a, first + b : last + b]
            hit = (words & (1 << bit)) | far
        pen = jnp.where(hit == 0, PEN, PEN - LOST)
        pen_ref[place, x] = pen
        return pen

    totals, volume = bond_pass(rolled_ref, mine_ref, pen_of, square_ref, along_ref, across_ref, sums_ref, region, "volume")
    solid = jnp.where(nb_ref[REACH, cells : 2 * cells, first:last] == 0, 1.0, 0.0)
    volume = jnp.maximum(volume * solid, 1.0)
    inverse = 1.0 / volume
    dilatation = 3.0 * (totals * solid) / volume
    ratio_ref[0] = dilatation * inverse * (0.5 * BULK_TERM)
    ratio_ref[1] = inverse * (0.5 * SHEAR_TERM / HALF)
    cut_ratio(ratio_ref, to_odd_ref, to_even_ref, rows)
    volume_ref[0] = volume
    volume_ref[1] = solid
    copy.wait()


def forces(total, inner, rolled_ref, square_ref, along_ref, across_ref, scaled_ref, inverse_ref, rows):
    half = rows // 2
    mine = slice(half, half + rows)
    for x in range(3):
        scaled = scaled_ref[REACH, x + 3, mine]
        inverse = inverse_ref[REACH, x + 3, mine]
        here = [rolled_ref[REACH, f, x + 3, rows : 2 * rows] for f in range(3)]
        for bonds in CLASSES.values():
            for a, b, c, word, bit, backward, place in bonds:
                if (0 <= x + a < 3) != inner:
                    continue
                far = (c + REACH, x + 3 + a, slice(half + b, half + rows + b))
                magnitude = along_ref[place, x, mine] * (scaled + scaled_ref[far])
                magnitude = magnitude + across_ref[place, x, mine] * (inverse + inverse_ref[far])
                magnitude = magnitude * lax.rsqrt(square_ref[place, x, mine] + DIRECTION_EPS)
                for f, step in enumerate((a, b, c)):
                    rel = rolled_ref[c + REACH, f, x + 3 + a, rows + b : 2 * rows + b] - here[f]
                    if step:
                        rel = rel + float(step)
                    total[f][x] = total[f][x] + magnitude * rel
    return total


def fill_inner(target_ref, own):
    for c in range(-REACH, REACH + 1):
        target_ref[c + REACH, 3:6] = shifted(own, c)


def fill_outer(target_ref, field_ref, f, odd_ref, even_ref, rows):
    even = is_even("gx")
    half = rows // 2
    field_ref[...] = jnp.zeros(field_ref.shape, F32)
    start = f * ratio_rows(rows)
    for distance in range(1, 4):
        count = rows + 2 * outer_rows(distance)
        part = slice(half - outer_rows(distance), half + rows + outer_rows(distance))
        from_odd, from_even = odd_ref[start : start + count], even_ref[start : start + count]
        field_ref[3 - distance, part] = jnp.where(even, from_odd, from_even)
        field_ref[2 + distance, part] = jnp.where(even, from_even, from_odd)
        start += count
    field = field_ref[...]
    for c in range(-REACH, REACH + 1):
        part = outer_part(c)
        if part is not None:
            turned = shifted(field[part], c)
            side = turned.shape[0] // 2
            target_ref[c + REACH, part.start : 3] = turned[:side]
            target_ref[c + REACH, 6 : 3 + part.stop] = turned[side:]


def start_total(rows, depth):
    return [[jnp.zeros((rows, depth), F32) for _ in range(3)] for _ in range(3)]


def inner_kernel(rolled_ref, square_ref, along_ref, across_ref, ratio_ref, held_ref, part_ref, scaled_ref, inverse_ref):
    rows, depth = part_ref.shape[2:]
    fill_inner(scaled_ref, ratio_ref[0])
    if held_ref is None:
        held_ref = inverse_ref
        fill_inner(inverse_ref, ratio_ref[1])
    total = forces(start_total(rows, depth), True, rolled_ref, square_ref, along_ref, across_ref, scaled_ref, held_ref, rows)
    for f in range(3):
        for x in range(3):
            part_ref[f, x] = total[f][x]


def first_inner_kernel(rolled_ref, square_ref, along_ref, across_ref, ratio_ref, part_ref, scaled_ref, inverse_ref):
    inner_kernel(rolled_ref, square_ref, along_ref, across_ref, ratio_ref, None, part_ref, scaled_ref, inverse_ref)


def outer_forces(rolled_ref, square_ref, along_ref, across_ref, scaled_ref, inverse_ref, part_ref, rows):
    total = [[part_ref[f, x] for x in range(3)] for f in range(3)]
    return forces(total, False, rolled_ref, square_ref, along_ref, across_ref, scaled_ref, inverse_ref, rows)


def move_kernel(rolled_ref, square_ref, along_ref, across_ref, ratio_ref, part_ref, odd_ref, even_ref, volume_ref, sent_ref, v_ref, u_out, v_out, inverse_ref, to_odd_ref, to_even_ref, scaled_ref, field_ref):
    rows = v_ref.shape[2]
    half = rows // 2
    for f, target in ((0, scaled_ref), (1, inverse_ref)):
        fill_outer(target, field_ref.at[f], f, odd_ref, even_ref, rows)
    scaled_ref[REACH, 3:6] = ratio_ref[0]
    fill_inner(inverse_ref, ratio_ref[1])
    total = outer_forces(rolled_ref, square_ref, along_ref, across_ref, scaled_ref, inverse_ref, part_ref, rows)
    for f in range(3):
        for x in range(3):
            speed = v_ref[f, x] + TIME_STEP * (total[f][x] * volume_ref[1, x, half : half + rows])
            v_out[f, x] = speed
            u_out[f, x] = sent_ref[3 * f + x] + TIME_STEP * speed
    cut_y(lambda f, x: u_out[f, x], 3, to_odd_ref, to_even_ref)


def strips_x(fields, rows, beyond):
    placed, start = {}, 0
    for f in range(fields):
        for distance in range(1, 4):
            if f >= 4 and word_reach()[f - 4] < distance:
                continue
            count = rows + 2 * beyond[distance]
            placed[f, distance] = (start, count, beyond[distance])
            start += count
    return placed, start


def cut_y(value_of, fields, odd_ref, even_ref):
    even = is_even("gy")
    for f in range(fields):
        for x in range(3):
            tile = value_of(f, x)
            first, last = tile[0:ROWS_Y], tile[tile.shape[0] - ROWS_Y :]
            part = slice((3 * f + x) * ROWS_Y, (3 * f + x + 1) * ROWS_Y)
            odd_ref[part] = jnp.where(even, first, last)
            even_ref[part] = jnp.where(even, last, first)


def cut_x(source_ref, fields, rows, beyond, base, odd_ref, even_ref):
    even = is_even("gx")
    for (f, distance), (start, count, more) in strips_x(fields, rows, beyond)[0].items():
        part = slice(base - more, base + rows + more)
        upper, lower = source_ref[f, 3 - distance, part], source_ref[f, distance - 1, part]
        odd_ref[start : start + count] = jnp.where(even, lower, upper)
        even_ref[start : start + count] = jnp.where(even, upper, lower)


def lay_side(field_ref, f, fields, rows, beyond, base, odd_ref, even_ref):
    even = is_even("gx")
    field_ref[...] = jnp.zeros(field_ref.shape, F32)
    placed = strips_x(fields, rows, beyond)[0]
    for distance in range(1, 4):
        if (f, distance) in placed:
            start, count, more = placed[f, distance]
            part = slice(base - more, base + rows + more)
            from_odd, from_even = odd_ref[start : start + count], even_ref[start : start + count]
            field_ref[3 - distance, part] = jnp.where(even, from_odd, from_even)
            field_ref[2 + distance, part] = jnp.where(even, from_even, from_odd)
    return field_ref[...]


def outer_part(c):
    return {0: slice(0, 6), 3: None}.get(abs(c), slice(1, 5))


def widen_moved_kernel(own_ref, odd_ref, even_ref, tall_ref, to_odd_ref, to_even_ref):
    even = is_even("gy")
    fields, rows = own_ref.shape[0], own_ref.shape[2]
    blank = jnp.zeros((rows - ROWS_Y, own_ref.shape[3]), F32)
    for f in range(fields):
        for x in range(3):
            part = slice((3 * f + x) * ROWS_Y, (3 * f + x + 1) * ROWS_Y)
            from_odd, from_even = odd_ref[part], even_ref[part]
            tall_ref[f, x, 0 : rows - ROWS_Y] = blank
            tall_ref[f, x, rows - ROWS_Y : rows] = jnp.where(even, from_odd, from_even)
            tall_ref[f, x, rows : 2 * rows] = own_ref[f, x]
            tall_ref[f, x, 2 * rows : 2 * rows + ROWS_Y] = jnp.where(even, from_even, from_odd)
            tall_ref[f, x, 2 * rows + ROWS_Y :] = blank
    cut_x(tall_ref, fields, rows, BEYOND, rows, to_odd_ref, to_even_ref)


def region_of(rows):
    return rows // 2, rows // 2 + 2 * rows


def split_pass(places, far_of, own_ref, pen_of, square_ref, along_ref, across_ref, sums_ref, begun_ref, kinds):
    shape = own_ref.shape[3:]
    for x in range(3):
        totals = jnp.zeros(shape, F32) if begun_ref is None else begun_ref[0, x]
        second = jnp.zeros(shape, F32) if begun_ref is None else begun_ref[1, x]
        for squared, bonds in CLASSES.items():
            natural = math.sqrt(squared)
            held = [bond for bond in bonds if (bond[-1], x) in places]
            if not held:
                continue
            moved = jnp.zeros(shape, F32)
            other = jnp.zeros(shape, F32)
            for bond in held:
                a, b, c = bond[:3]
                n = places[bond[-1], x]
                rel = [far_of(c, f, x + a, b) - own_ref[f, step + REACH, x] for f, step in enumerate((a, b, c))]
                square = rel[0] * rel[0] + rel[1] * rel[1] + rel[2] * rel[2]
                length = square * lax.rsqrt(jnp.maximum(square, 1e-30))
                scaled = (length - natural) * (HALF / natural)
                pen = pen_of(bond, n, x)
                weight = 1.0 + jnp.tanh(pen - scaled)
                pulled = weight * scaled
                square_ref[n] = square
                along_ref[n] = weight
                across_ref[n] = pulled
                moved = moved + pulled
                other = other + (pen if kinds == "volume" else weight)
            totals = totals + moved * (0.5 * natural / HALF)
            if kinds == "volume":
                lost = (PEN * len(held) - other) * (1.0 / LOST)
                second = second + (len(held) - lost) * natural
            else:
                second = second + other * (0.5 * natural)
        sums_ref[0, x] = totals
        sums_ref[1, x] = second


def fill_inner_moving(tall_ref, rolled_ref, mine_ref):
    first, last = region_of(tall_ref.shape[2] // 3)
    for f in range(3):
        field = tall_ref[f]
        for c in range(-REACH, REACH + 1):
            rolled_ref[c + REACH, f] = shifted(field, c)
        here = tall_ref[f, :, first:last]
        for step in range(-REACH, REACH + 1):
            mine_ref[f, step + REACH] = here - float(step)


def fill_outer_moving(odd_ref, even_ref, fields, field_ref, rolled_ref):
    rows = field_ref.shape[2] // 3
    for f in range(3):
        field = lay_side(field_ref.at[f], f, fields, rows, BEYOND, rows, odd_ref, even_ref)
        for c in range(-REACH, REACH + 1):
            part = outer_part(c)
            if part is not None:
                rolled_ref[c + REACH, f, part] = shifted(field[part], c)


def inner_far(rolled_ref):
    first, last = region_of(rolled_ref.shape[3] // 3)
    return lambda c, f, layer, b: rolled_ref[c + REACH, f, layer, first + b : last + b]


def outer_far(rolled_ref):
    first, last = region_of(rolled_ref.shape[3] // 3)
    return lambda c, f, layer, b: rolled_ref[c + REACH, f, SIDE.index(layer), first + b : last + b]


def later_inside_kernel(tall_ref, pen_ref, rolled_ref, mine_ref, square_ref, along_ref, across_ref, sums_ref):
    fill_inner_moving(tall_ref, rolled_ref, mine_ref)
    split_pass(INNER, inner_far(rolled_ref), mine_ref, lambda bond, n, x: pen_ref[bond[-1], x], square_ref, along_ref, across_ref, sums_ref, None, "weight")


def later_kernel(odd_ref, even_ref, mine_ref, pen_ref, begun_ref, volume_ref, rolled_ref, square_ref, along_ref, across_ref, ratio_ref, to_odd_ref, to_even_ref, damage_ref, field_ref, sums_ref):
    rows = field_ref.shape[2] // 3
    half = rows // 2
    fill_outer_moving(odd_ref, even_ref, 3, field_ref, rolled_ref)
    split_pass(OUTER, outer_far(rolled_ref), mine_ref, lambda bond, n, x: pen_ref[bond[-1], x], square_ref, along_ref, across_ref, sums_ref, begun_ref, "weight")
    volume = volume_ref[0]
    solid = volume_ref[1]
    inverse = 1.0 / volume
    dilatation = 3.0 * (sums_ref[0] * solid) / volume
    ratio_ref[0] = dilatation * inverse * (0.5 * BULK_TERM)
    cut_x(ratio_ref, 1, rows, BEYOND_RATIO, half, to_odd_ref, to_even_ref)
    damage = 1.0 - (sums_ref[1] * solid) / volume
    damage_ref[...] = damage[:, half : half + rows]


def split_forces(total, places, index, rolled_ref, here_ref, square_ref, along_ref, across_ref, ratio_ref, held_ref, scaled_ref, inverse_ref):
    rows = here_ref.shape[3] // 3
    half = rows // 2
    mine = slice(half, half + rows)
    for x in range(3):
        scaled = ratio_ref[0, x, mine]
        inverse = held_ref[1, x, mine]
        here = [here_ref[REACH, f, x, rows : 2 * rows] for f in range(3)]
        for a, b, c, word, bit, backward, place in DIRECTED:
            if (place, x) not in places:
                continue
            n = places[place, x]
            far = (c + REACH, index(x + a), slice(half + b, half + rows + b))
            magnitude = along_ref[n, mine] * (scaled + scaled_ref[far])
            magnitude = magnitude + across_ref[n, mine] * (inverse + inverse_ref[c + REACH, x + 3 + a, far[2]])
            magnitude = magnitude * lax.rsqrt(square_ref[n, mine] + DIRECTION_EPS)
            for f, step in enumerate((a, b, c)):
                rel = rolled_ref[c + REACH, f, index(x + a), rows + b : 2 * rows + b] - here[f]
                if step:
                    rel = rel + float(step)
                total[f][x] = total[f][x] + magnitude * rel
    return total


def fill_own(target_ref, own):
    for c in range(-REACH, REACH + 1):
        target_ref[c + REACH] = shifted(own, c)


def fill_side(target_ref, field_ref, f, fields, odd_ref, even_ref, rows):
    field = lay_side(field_ref, f, fields, rows, BEYOND_RATIO, rows // 2, odd_ref, even_ref)
    for c in range(-REACH, REACH + 1):
        part = outer_part(c)
        if part is not None:
            target_ref[c + REACH, part] = shifted(field[part], c)


def inside_forces(rolled_ref, square_ref, along_ref, across_ref, ratio_ref, held_ref, scaled_ref, inverse_ref, part_ref):
    rows, depth = part_ref.shape[2:]
    total = [[jnp.zeros((rows, depth), F32) for _ in range(3)] for _ in range(3)]
    total = split_forces(total, INNER, lambda layer: layer, rolled_ref, rolled_ref, square_ref, along_ref, across_ref, ratio_ref, held_ref, scaled_ref, inverse_ref)
    for f in range(3):
        for x in range(3):
            part_ref[f, x] = total[f][x]


def last_inside_kernel(rolled_ref, square_ref, along_ref, across_ref, ratio_ref, held_ref, inverse_ref, part_ref, scaled_ref):
    fill_own(scaled_ref, ratio_ref[0])
    inside_forces(rolled_ref, square_ref, along_ref, across_ref, ratio_ref, held_ref, scaled_ref, inverse_ref, part_ref)


def last_kernel(odd_ref, even_ref, rolled_ref, inside_ref, square_ref, along_ref, across_ref, ratio_ref, held_ref, part_ref, volume_ref, v_ref, inverse_ref, damage_ref, v_out, damage_out, scaled_ref, field_ref):
    rows = v_ref.shape[2]
    half = rows // 2
    damage_out[...] = damage_ref[...]
    fill_side(scaled_ref, field_ref, 0, 1, odd_ref, even_ref, rows)
    total = [[part_ref[f, x] for x in range(3)] for f in range(3)]
    total = split_forces(total, OUTER, SIDE.index, rolled_ref, inside_ref, square_ref, along_ref, across_ref, ratio_ref, held_ref, scaled_ref, inverse_ref)
    for f in range(3):
        for x in range(3):
            v_out[f, x] = v_ref[f, x] + TIME_STEP * (total[f][x] * volume_ref[1, x, half : half + rows])


def body(displacement, velocity, bone, broken):
    cells, rows, depth = bone.shape
    if cells != REACH or rows != 8:
        raise ValueError("block size")
    layers, tall, region = 3 * cells, 3 * rows, 2 * rows
    turns = 2 * REACH + 1

    def vmem(*shape, dtype=F32):
        return pltpu.VMEM(shape, dtype)

    hbm = jax.ShapeDtypeStruct
    sent, kept = call(
        pack_kernel,
        (vmem(len(SENT), rows, depth), vmem(len(KEPT), rows, depth)),
        displacement,
        bone,
        broken,
        scratch=(
            vmem(cells, rows, depth, dtype=jnp.int32),
            vmem(4, cells, rows, depth, dtype=jnp.int32),
            pltpu.SemaphoreType.DMA((5,)),
        ),
        hbm=(0, 1, 2),
    )
    side, to_odd, to_even = call(
        widen_kernel,
        (vmem(2, len(SENT), rows, depth), vmem(ALL_ROWS, depth), vmem(ALL_ROWS, depth)),
        sent,
        kept,
        *both(sent, sent, "gx"),
    )
    bonds = (BONDS, cells, region, depth)
    crossing = ratio_rows(rows)
    rolled, pen, square, along, across, ratio, to_odd, to_even, volume, speed = call(
        first_kernel,
        (
            vmem(turns, 3, layers, tall, depth),
            vmem(*bonds),
            vmem(*bonds),
            vmem(*bonds),
            vmem(*bonds),
            vmem(2, cells, region, depth),
            vmem(2 * crossing, depth),
            vmem(2 * crossing, depth),
            vmem(2, cells, region, depth),
            vmem(3, cells, rows, depth),
        ),
        side,
        sent,
        kept,
        *both(to_odd, to_even, "gy"),
        velocity,
        scratch=(
            vmem(3, turns, cells, region, depth),
            vmem(3, layers, tall, depth),
            vmem(turns, layers, tall, depth, dtype=jnp.int32),
            vmem(turns, 4, 2 * cells, tall, depth, dtype=jnp.int32),
            vmem(2, cells, region, depth),
            pltpu.SemaphoreType.DMA(()),
        ),
        hbm=(5,),
    )
    arrived = both(to_odd, to_even, "gx")
    wide_ratio = vmem(turns, layers, region, depth)
    part = call(
        first_inner_kernel,
        vmem(3, cells, rows, depth),
        rolled,
        square,
        along,
        across,
        ratio,
        scratch=(wide_ratio, wide_ratio),
    )
    moved, speed, inverse, *to = call(
        move_kernel,
        (vmem(3, cells, rows, depth), vmem(3, cells, rows, depth), wide_ratio) + (vmem(3 * 3 * ROWS_Y, depth),) * 2,
        rolled,
        square,
        along,
        across,
        ratio,
        part,
        *arrived,
        volume,
        sent,
        speed,
        scratch=(wide_ratio, vmem(2, 6, region, depth)),
    )
    sides = len(SIDE)
    block = vmem(3, cells, rows, depth)
    in_bonds, out_bonds = vmem(len(INNER), region, depth), vmem(len(OUTER), region, depth)
    in_rolled, out_rolled = vmem(turns, 3, cells, tall, depth), vmem(turns, 3, sides, tall, depth)
    in_ratio, out_ratio = vmem(turns, cells, region, depth), vmem(turns, sides, region, depth)
    mine_shape = vmem(3, turns, cells, region, depth)
    two = vmem(2, cells, region, depth)

    def strips(fields, beyond):
        return (vmem(strips_x(fields, rows, beyond)[1], depth),) * 2

    tall_moved, *to = call(
        widen_moved_kernel, (vmem(3, cells, tall, depth),) + strips(3, BEYOND), moved, *both(*to, "gy")
    )
    arrived = both(*to, "gx")
    inside, mine, *in_held, begun = call(
        later_inside_kernel, (in_rolled, mine_shape) + (in_bonds,) * 3 + (two,), tall_moved, pen
    )
    held_ratio = ratio
    rolled, *out_held, ratio, to_odd, to_even, damage = call(
        later_kernel,
        (out_rolled,) + (out_bonds,) * 3 + (vmem(1, cells, region, depth),) + strips(1, BEYOND_RATIO) + (vmem(cells, rows, depth),),
        *arrived,
        mine,
        pen,
        begun,
        volume,
        scratch=(vmem(3, sides, tall, depth), two),
    )
    arrived = both(to_odd, to_even, "gx")
    part = call(last_inside_kernel, block, inside, *in_held, ratio, held_ratio, inverse, scratch=(in_ratio,))
    return call(
        last_kernel,
        (hbm((3, cells, rows, depth), F32), hbm((cells, rows, depth), F32)),
        *arrived,
        rolled,
        inside,
        *out_held,
        ratio,
        held_ratio,
        part,
        volume,
        speed,
        inverse,
        damage,
        scratch=(out_ratio, vmem(sides, region, depth)),
    )


def solution(mesh):
    in_specs = (
        P(None, "gx", "gy", None),
        P(None, "gx", "gy", None),
        P("gx", "gy", None),
        P(None, "gx", "gy", None),
    )
    out_specs = (P(None, "gx", "gy", None), P("gx", "gy", None))
    return jax.shard_map(body, mesh=mesh, in_specs=in_specs, out_specs=out_specs, check_vma=False)
```
